16 devices in a mesh: rep: 1, dp: 16 (over x, y, z, core).
Axes of the slice: x: 2, y: 2, z: 2, core: 2. Of those that a mesh axis runs over, the one named last changes fastest.
Arguments:
- x: bfloat16 [16, 2048, 512], P(('rep', 'dp'))
- dy: bfloat16 [16, 2048, 512], P(('rep', 'dp'))
- w_gate: bfloat16 [2, 512, 4096], replicated
- w_up: bfloat16 [2, 512, 4096], replicated
- w_down: bfloat16 [2, 4096, 512], replicated
- m_w_gate: float32 [2, 512, 4096], replicated
- m_w_up: float32 [2, 512, 4096], replicated
- m_w_down: float32 [2, 4096, 512], replicated
- v_w_gate: float32 [2, 512, 4096], replicated
- v_w_up: float32 [2, 512, 4096], replicated
- v_w_down: float32 [2, 4096, 512], replicated
Outputs:
- output 1: bfloat16 [2, 512, 4096], P('rep')
- output 2: bfloat16 [2, 512, 4096], P('rep')
- output 3: bfloat16 [2, 4096, 512], P('rep')
- output 4: float32 [2, 512, 4096], P('rep')
- output 5: float32 [2, 512, 4096], P('rep')
- output 6: float32 [2, 4096, 512], P('rep')
- output 7: float32 [2, 512, 4096], P('rep')
- output 8: float32 [2, 512, 4096], P('rep')
- output 9: float32 [2, 4096, 512], P('rep')
All inputs are finite; a program needn't handle non-finite values.
Results may differ from the reference program's by a relative error of at most 0.022.
Values are sent between devices in bfloat16 or wider.
A program may use at most 2.5 GiB of HBM per device.

```python
import jax
import jax.numpy as jnp
from jax import lax

SEQUENCES = 16
TOKENS = 2048
D = 512
FF = 4096
LAYERS = 2
NAMES = ("w_gate", "w_up", "w_down")
SHAPES = {"w_gate": (LAYERS, D, FF), "w_up": (LAYERS, D, FF), "w_down": (LAYERS, FF, D)}


def bump(key, n, height):
    away = (jnp.arange(n, dtype=jnp.int32) - jax.random.randint(key, (), 0, n, jnp.int32)) % n
    return jnp.where(away < n // 8, height, 1.0)


def together(key, own, strength):
    shared = jax.random.normal(key, own.shape[1:], jnp.float32)
    return (own + strength * shared) * lax.rsqrt(1 + strength * strength)


def setup_inputs(seed: int = 0, part: int = 0) -> dict:
    kx, kdy, ka, kb, kz, kf, kh, kl, *keys = jax.random.split(jax.random.key(seed), 8 + 3 * len(NAMES))
    kx, kdy, ka, kb = (jax.random.fold_in(k, part) for k in (kx, kdy, ka, kb))
    kw, km, kv = (keys[i::3] for i in range(3))
    shape = (SEQUENCES, TOKENS, D)
    much_x, much_dy = jax.random.uniform(kz, (2,), jnp.float32, 0.0, 1.0)
    loud = 2.0 ** jax.random.uniform(jax.random.fold_in(kz, 1), (), jnp.float32, -1.0, 2.0)
    layers = 2.0 ** jax.random.uniform(kl, (LAYERS, 1, 1), jnp.float32, -1.0, 1.0)
    x = together(ka, jax.random.normal(kx, shape, jnp.float32), much_x) * bump(kf, D, 4.0)
    dy = together(kb, jax.random.normal(kdy, shape, jnp.float32), much_dy)
    drawn = {"x": x.astype(jnp.bfloat16), "dy": (loud * dy * (SEQUENCES * TOKENS) ** -0.5).astype(jnp.bfloat16)}
    for key, name in zip(kw, NAMES, strict=True):
        w = jax.random.normal(key, SHAPES[name], jnp.float32) * SHAPES[name][1] ** -0.5
        drawn[name] = (w * {"w_gate": 1.0, "w_up": bump(kh, FF, 4.0), "w_down": layers}[name]).astype(jnp.bfloat16)
    for key, name in zip(km, NAMES, strict=True):
        drawn[f"m_{name}"] = 0.1 * jax.random.normal(key, SHAPES[name], jnp.float32)
    for key, name in zip(kv, NAMES, strict=True):
        drawn[f"v_{name}"] = jax.random.uniform(key, SHAPES[name], jnp.float32, 0.005, 0.015)
    return drawn


def matmul(a, w):
    return jnp.dot(a, w, preferred_element_type=jnp.float32).astype(jnp.bfloat16)


def normed(h):
    wide = h.astype(jnp.float32)
    scale = lax.rsqrt(jnp.mean(wide**2, -1, keepdims=True) + 1e-6)
    return (wide * scale).astype(jnp.bfloat16)


def layer(h, w):
    a = normed(h)
    gate = jnp.dot(a, w["w_gate"], preferred_element_type=jnp.float32)
    up = jnp.dot(a, w["w_up"], preferred_element_type=jnp.float32)
    return h + matmul((jax.nn.silu(gate) * up).astype(jnp.bfloat16), w["w_down"])


def adamw(w, m, v, g):
    m = 0.9 * m + 0.1 * g
    v = 0.95 * v + 0.05 * g * g
    step = m * lax.rsqrt(v + 1e-8) + 0.1 * w
    return (w - 0.02 * step).astype(jnp.bfloat16), m, v


def clipped(gradients, sum_of_squares, count):
    factor = jnp.minimum(1.0, 0.5 * lax.rsqrt(sum_of_squares / count + 1e-30))
    return [g * factor for g in gradients]


def stack(weights, h):
    return lax.scan(lambda h, w: (layer(h, w), None), h, weights)[0]


def reference(x, dy, w_gate, w_up, w_down, m_w_gate, m_w_up, m_w_down, v_w_gate, v_w_up, v_w_down):
    weights = dict(zip(NAMES, (w_gate, w_up, w_down), strict=True))

    def take(so_far, sequence):
        h, by_y = sequence
        _, back = jax.vjp(lambda w: stack(w, h), weights)
        return jax.tree.map(lambda total, term: total + term.astype(jnp.float32), so_far, back(by_y)[0]), None

    none_yet = {name: jnp.zeros(w.shape, jnp.float32) for name, w in weights.items()}
    by_weights, _ = lax.scan(take, none_yet, (x, dy))
    gradients = [by_weights[name].astype(jnp.bfloat16).astype(jnp.float32) for name in NAMES]
    gradients = clipped(gradients, sum(jnp.sum(g * g) for g in gradients), sum(g.size for g in gradients))
    new = [
        adamw(w.astype(jnp.float32), m, v, g)
        for w, m, v, g in zip((w_gate, w_up, w_down), (m_w_gate, m_w_up, m_w_down), (v_w_gate, v_w_up, v_w_down), gradients, strict=True)
    ]
    return tuple(one[which] for which in range(3) for one in new)
```

```python
import functools
import jax
import jax.numpy as jnp
from jax import lax
from jax.experimental import pallas as pl
from jax.experimental.pallas import tpu as pltpu
from jax.sharding import PartitionSpec as P

F32, BF16 = jnp.float32, jnp.bfloat16
VMEM_LIMIT = 67_000_000


def dot(a, b, da, db):
    return lax.dot_general(a, b, (((da,), (db,)), ((), ())), preferred_element_type=F32)


def norm_scale(wide):
    return lax.rsqrt(jnp.mean(wide * wide, -1, keepdims=True) + 1e-6)


def sigmoid(g):
    return 1.0 / (1.0 + jnp.exp(-g))


def forward_kernel(tb, x_ref, wg_ref, wu_ref, wd_ref, gate_ref, up_ref, h_ref, a_ref, at_ref, acc_ref):
    f, last = pl.program_id(0), pl.num_programs(0) - 1
    tokens = acc_ref.shape[0]

    @pl.when(f == 0)
    def _():
        for t in range(0, tokens, tb):
            rows = pl.ds(t, tb)
            wide = x_ref[0, rows, :].astype(F32)
            a = (wide * norm_scale(wide)).astype(BF16)
            a_ref[rows, :] = a
            at_ref[:, rows] = a.T
            acc_ref[rows, :] = jnp.zeros((tb, acc_ref.shape[1]), F32)

    for t in range(0, tokens, tb):
        rows = pl.ds(t, tb)
        a = a_ref[rows, :]
        gate = dot(a, wg_ref[0], 1, 0)
        up = dot(a, wu_ref[0], 1, 0)
        gate_ref[rows, :] = gate
        up_ref[rows, :] = up
        hid = (gate * sigmoid(gate) * up).astype(BF16)
        acc_ref[rows, :] += dot(hid, wd_ref[0], 1, 0)

    @pl.when(f == last)
    def _():
        for t in range(0, tokens, tb):
            rows = pl.ds(t, tb)
            h_ref[rows, :] = (x_ref[0, rows, :].astype(F32) + acc_ref[rows, :].astype(BF16).astype(F32)).astype(BF16)


def forward(x, wg, wu, wd, fb=256, tb=512):
    _, tokens, d = x.shape
    ff = wg.shape[2]
    whole = lambda *s: pl.BlockSpec(s, lambda f: (0,) * len(s))
    return pl.pallas_call(
        functools.partial(forward_kernel, tb),
        grid=(ff // fb,),
        in_specs=[
            whole(1, tokens, d),
            pl.BlockSpec((1, d, fb), lambda f: (0, 0, f)),
            pl.BlockSpec((1, d, fb), lambda f: (0, 0, f)),
            pl.BlockSpec((1, fb, d), lambda f: (0, f, 0)),
        ],
        out_specs=[
            pl.BlockSpec((tokens, fb), lambda f: (0, f)),
            pl.BlockSpec((tokens, fb), lambda f: (0, f)),
            whole(tokens, d),
            whole(tokens, d),
            whole(d, tokens),
        ],
        out_shape=[
            jax.ShapeDtypeStruct((tokens, ff), F32),
            jax.ShapeDtypeStruct((tokens, ff), F32),
            jax.ShapeDtypeStruct((tokens, d), BF16),
            jax.ShapeDtypeStruct((tokens, d), BF16),
            jax.ShapeDtypeStruct((d, tokens), BF16),
        ],
        scratch_shapes=[pltpu.VMEM((tokens, d), F32)],
        compiler_params=pltpu.CompilerParams(vmem_limit_bytes=VMEM_LIMIT),
        cost_estimate=pl.CostEstimate(flops=6 * tokens * d * ff, bytes_accessed=9 * tokens * ff, transcendentals=0),
        name="forward",
    )(x, wg, wu, wd)


def top_kernel(tb, h_ref, dy_ref, wg_ref, wu_ref, wd_ref, dwg_ref, dwu_ref, dwd_ref, dh_ref,
               a_ref, at_ref, dyt_ref, by_gate, by_up, hid_ref, dgate_ref, dup_ref):
    f, last = pl.program_id(0), pl.num_programs(0) - 1
    tokens, d = a_ref.shape

    @pl.when(f == 0)
    def _():
        for t in range(0, tokens, tb):
            rows = pl.ds(t, tb)
            wide = h_ref[rows, :].astype(F32)
            a = (wide * norm_scale(wide)).astype(BF16)
            a_ref[rows, :] = a
            at_ref[:, rows] = a.T
            dyt_ref[:, rows] = dy_ref[0, rows, :].T
            by_gate[rows, :] = jnp.zeros((tb, d), F32)
            by_up[rows, :] = jnp.zeros((tb, d), F32)

    for t in range(0, tokens, tb):
        rows = pl.ds(t, tb)
        a = a_ref[rows, :]
        gate = dot(a, wg_ref[0], 1, 0)
        up = dot(a, wu_ref[0], 1, 0)
        dhid = dot(dy_ref[0, rows, :], wd_ref[0], 1, 1).astype(BF16).astype(F32)
        s = sigmoid(gate)
        silu = gate * s
        hid_ref[rows, :] = (silu * up).astype(BF16)
        dup = (dhid * silu).astype(BF16)
        dgate = (dhid * up * (s + silu * (1.0 - s))).astype(BF16)
        dup_ref[rows, :] = dup
        dgate_ref[rows, :] = dgate
        by_gate[rows, :] += dot(dgate, wg_ref[0], 1, 1)
        by_up[rows, :] += dot(dup, wu_ref[0], 1, 1)

    dwg_ref[...] = dot(at_ref[...], dgate_ref[...], 1, 0).astype(BF16)
    dwu_ref[...] = dot(at_ref[...], dup_ref[...], 1, 0).astype(BF16)
    dwd_ref[...] = dot(dyt_ref[...], hid_ref[...], 1, 0).T.astype(BF16)

    @pl.when(f == last)
    def _():
        for t in range(0, tokens, tb):
            rows = pl.ds(t, tb)
            wide = h_ref[rows, :].astype(F32)
            scale = norm_scale(wide)
            da = (by_gate[rows, :].astype(BF16).astype(F32) + by_up[rows, :].astype(BF16).astype(F32)).astype(BF16).astype(F32)
            dn = scale * da - wide * (scale * scale * scale * jnp.mean(da * wide, -1, keepdims=True))
            dh_ref[rows, :] = (dy_ref[0, rows, :].astype(F32) + dn.astype(BF16).astype(F32)).astype(BF16)


def top(h, dy, wg, wu, wd, fb=256, tb=512):
    tokens, d = h.shape
    ff = wg.shape[2]
    whole = lambda *s: pl.BlockSpec(s, lambda f: (0,) * len(s))
    return pl.pallas_call(
        functools.partial(top_kernel, tb),
        grid=(ff // fb,),
        in_specs=[
            whole(tokens, d),
            whole(1, tokens, d),
            pl.BlockSpec((1, d, fb), lambda f: (1, 0, f)),
            pl.BlockSpec((1, d, fb), lambda f: (1, 0, f)),
            pl.BlockSpec((1, fb, d), lambda f: (1, f, 0)),
        ],
        out_specs=[
            pl.BlockSpec((d, fb), lambda f: (0, f)),
            pl.BlockSpec((d, fb), lambda f: (0, f)),
            pl.BlockSpec((fb, d), lambda f: (f, 0)),
            whole(tokens, d),
        ],
        out_shape=[
            jax.ShapeDtypeStruct((d, ff), BF16),
            jax.ShapeDtypeStruct((d, ff), BF16),
            jax.ShapeDtypeStruct((ff, d), BF16),
            jax.ShapeDtypeStruct((tokens, d), BF16),
        ],
        scratch_shapes=[
            pltpu.VMEM((tokens, d), BF16),
            pltpu.VMEM((d, tokens), BF16),
            pltpu.VMEM((d, tokens), BF16),
            pltpu.VMEM((tokens, d), F32),
            pltpu.VMEM((tokens, d), F32),
            pltpu.VMEM((tokens, fb), BF16),
            pltpu.VMEM((tokens, fb), BF16),
            pltpu.VMEM((tokens, fb), BF16),
        ],
        compiler_params=pltpu.CompilerParams(vmem_limit_bytes=VMEM_LIMIT),
        cost_estimate=pl.CostEstimate(flops=16 * tokens * d * ff, bytes_accessed=20 * d * ff, transcendentals=0),
        name="top",
    )(h, dy, wg, wu, wd)


def bottom_kernel(tb, dh_ref, at_ref, gate_ref, up_ref, wd_ref, dwg_ref, dwu_ref, dwd_ref, dht_ref, hid_ref, dgate_ref, dup_ref):
    f = pl.program_id(0)
    tokens = dh_ref.shape[0]

    @pl.when(f == 0)
    def _():
        for t in range(0, tokens, tb):
            rows = pl.ds(t, tb)
            dht_ref[:, rows] = dh_ref[rows, :].T

    for t in range(0, tokens, tb):
        rows = pl.ds(t, tb)
        gate, up = gate_ref[rows, :], up_ref[rows, :]
        dhid = dot(dh_ref[rows, :], wd_ref[0], 1, 1).astype(BF16).astype(F32)
        s = sigmoid(gate)
        silu = gate * s
        hid_ref[rows, :] = (silu * up).astype(BF16)
        dup_ref[rows, :] = (dhid * silu).astype(BF16)
        dgate_ref[rows, :] = (dhid * up * (s + silu * (1.0 - s))).astype(BF16)

    dwg_ref[...] = dot(at_ref[...], dgate_ref[...], 1, 0).astype(BF16)
    dwu_ref[...] = dot(at_ref[...], dup_ref[...], 1, 0).astype(BF16)
    dwd_ref[...] = dot(dht_ref[...], hid_ref[...], 1, 0).T.astype(BF16)


def bottom(dh, at, gate, up, wd, fb=256, tb=512):
    tokens, d = dh.shape
    ff = wd.shape[1]
    whole = lambda *s: pl.BlockSpec(s, lambda f: (0,) * len(s))
    return pl.pallas_call(
        functools.partial(bottom_kernel, tb),
        grid=(ff // fb,),
        in_specs=[
            whole(tokens, d),
            whole(d, tokens),
            pl.BlockSpec((tokens, fb), lambda f: (0, f)),
            pl.BlockSpec((tokens, fb), lambda f: (0, f)),
            pl.BlockSpec((1, fb, d), lambda f: (0, f, 0)),
        ],
        out_specs=[
            pl.BlockSpec((d, fb), lambda f: (0, f)),
            pl.BlockSpec((d, fb), lambda f: (0, f)),
            pl.BlockSpec((fb, d), lambda f: (f, 0)),
        ],
        out_shape=[
            jax.ShapeDtypeStruct((d, ff), BF16),
            jax.ShapeDtypeStruct((d, ff), BF16),
            jax.ShapeDtypeStruct((ff, d), BF16),
        ],
        scratch_shapes=[
            pltpu.VMEM((d, tokens), BF16),
            pltpu.VMEM((tokens, fb), BF16),
            pltpu.VMEM((tokens, fb), BF16),
            pltpu.VMEM((tokens, fb), BF16),
        ],
        compiler_params=pltpu.CompilerParams(vmem_limit_bytes=VMEM_LIMIT),
        cost_estimate=pl.CostEstimate(flops=8 * tokens * d * ff, bytes_accessed=9 * tokens * ff, transcendentals=0),
        name="bottom",
    )(dh, at, gate, up, wd)


def adamw_kernel(factor_ref, *refs):
    ins, outs = refs[:12], refs[12:]
    factor = factor_ref[0, 0]
    for i in range(3):
        w, m, v, g = (ins[4 * i + j] for j in range(4))
        g = g[...].astype(F32) * factor
        m = 0.9 * m[...] + 0.1 * g
        v = 0.95 * v[...] + 0.05 * g * g
        w = w[...].astype(F32)
        w = w - 0.02 * (m * lax.rsqrt(v + 1e-8) + 0.1 * w)
        outs[i][...] = w.astype(BF16)
        outs[3 + i][...] = m
        outs[6 + i][...] = v


def adamw(factor, ws, ms, vs, gs, steps=16):
    specs = []
    for w in ws:
        layers, r, c = w.shape
        specs.append(pl.BlockSpec((1, r // steps, c), lambda l, f: (l, f, 0)))
    ins, in_specs = [], []
    for w, m, v, g, spec in zip(ws, ms, vs, gs, specs):
        ins += [w, m, v, g]
        in_specs += [spec] * 4
    shapes = [jax.ShapeDtypeStruct(w.shape, t) for t in (BF16, F32, F32) for w in ws]
    return pl.pallas_call(
        adamw_kernel,
        grid=(ws[0].shape[0], steps),
        in_specs=[pl.BlockSpec(memory_space=pltpu.SMEM)] + in_specs,
        out_specs=specs * 3,
        out_shape=shapes,
        compiler_params=pltpu.CompilerParams(vmem_limit_bytes=VMEM_LIMIT),
        cost_estimate=pl.CostEstimate(flops=20 * 3 * ws[0].size, bytes_accessed=22 * 3 * ws[0].size, transcendentals=0),
        name="adamw",
    )(factor, *ins)


def solution(mesh):
    def step(x, dy, *arrays):
        ws, ms, vs = (arrays[i : i + 3] for i in (0, 3, 6))
        gate, up, h, _, at = forward(x, *ws)
        *top_g, dh = top(h, dy, *ws)
        top_g = lax.psum(top_g, "dp")
        bottom_g = bottom(dh, at, gate, up, ws[2])
        bottom_g = lax.psum(bottom_g, "dp")
        gs = [jnp.stack(pair) for pair in zip(bottom_g, top_g)]
        total = sum(jnp.sum(g.astype(F32) ** 2) for g in gs)
        factor = jnp.minimum(1.0, 0.5 * lax.rsqrt(total / sum(g.size for g in gs) + 1e-30))
        return tuple(adamw(factor.reshape(1, 1), ws, ms, vs, gs))

    return jax.shard_map(
        step,
        mesh=mesh,
        in_specs=(P(("rep", "dp"), None, None),) * 2 + (P(None, None, None),) * 9,
        out_specs=(P("rep", None, None),) * 9,
        check_vma=False,
    )
```

```python
import functools
import jax
import jax.numpy as jnp
from jax import lax
from jax.experimental import pallas as pl
from jax.experimental.pallas import tpu as pltpu
from jax.sharding import PartitionSpec as P

F32, BF16 = jnp.float32, jnp.bfloat16
VMEM_LIMIT = 67_000_000


def dot(a, b, da, db):
    return lax.dot_general(a, b, (((da,), (db,)), ((), ())), preferred_element_type=F32)


def norm_scale(wide):
    return lax.rsqrt(jnp.mean(wide * wide, -1, keepdims=True) + 1e-6)


def sigmoid(g):
    return 1.0 / (1.0 + jnp.exp(-g))


def forward_kernel(tb, x_ref, wg_ref, wu_ref, wd_ref, gate_ref, up_ref, h_ref, at_ref, a_ref, acc_ref):
    f, last = pl.program_id(0), pl.num_programs(0) - 1
    tokens = acc_ref.shape[0]

    @pl.when(f == 0)
    def _():
        for t in range(0, tokens, tb):
            rows = pl.ds(t, tb)
            wide = x_ref[0, rows, :].astype(F32)
            a = (wide * norm_scale(wide)).astype(BF16)
            a_ref[rows, :] = a
            at_ref[:, rows] = a.T
            acc_ref[rows, :] = jnp.zeros((tb, acc_ref.shape[1]), F32)

    for t in range(0, tokens, tb):
        rows = pl.ds(t, tb)
        a = a_ref[rows, :]
        gate = dot(a, wg_ref[0], 1, 0)
        up = dot(a, wu_ref[0], 1, 0)
        gate_ref[rows, :] = gate
        up_ref[rows, :] = up
        hid = (gate * sigmoid(gate) * up).astype(BF16)
        acc_ref[rows, :] += dot(hid, wd_ref[0], 1, 0)

    @pl.when(f == last)
    def _():
        for t in range(0, tokens, tb):
            rows = pl.ds(t, tb)
            h_ref[rows, :] = (x_ref[0, rows, :].astype(F32) + acc_ref[rows, :].astype(BF16).astype(F32)).astype(BF16)


def forward(x, wg, wu, wd, fb=256, tb=512):
    _, tokens, d = x.shape
    ff = wg.shape[2]
    whole = lambda *s: pl.BlockSpec(s, lambda f: (0,) * len(s))
    return pl.pallas_call(
        functools.partial(forward_kernel, tb),
        grid=(ff // fb,),
        in_specs=[
            whole(1, tokens, d),
            pl.BlockSpec((1, d, fb), lambda f: (0, 0, f)),
            pl.BlockSpec((1, d, fb), lambda f: (0, 0, f)),
            pl.BlockSpec((1, fb, d), lambda f: (0, f, 0)),
        ],
        out_specs=[
            pl.BlockSpec((tokens, fb), lambda f: (0, f)),
            pl.BlockSpec((tokens, fb), lambda f: (0, f)),
            whole(tokens, d),
            whole(d, tokens),
        ],
        out_shape=[
            jax.ShapeDtypeStruct((tokens, ff), F32),
            jax.ShapeDtypeStruct((tokens, ff), F32),
            jax.ShapeDtypeStruct((tokens, d), BF16),
            jax.ShapeDtypeStruct((d, tokens), BF16),
        ],
        scratch_shapes=[pltpu.VMEM((tokens, d), BF16), pltpu.VMEM((tokens, d), F32)],
        compiler_params=pltpu.CompilerParams(vmem_limit_bytes=VMEM_LIMIT),
        cost_estimate=pl.CostEstimate(flops=6 * tokens * d * ff, bytes_accessed=9 * tokens * ff, transcendentals=0),
        name="forward",
    )(x, wg, wu, wd)


def adamw_kernel(factor_ref, *refs):
    ins, outs = refs[:12], refs[12:]
    factor = factor_ref[0:1, 0:1]
    for i in range(3):
        w, m, v, g = (ins[4 * i + j] for j in range(4))
        g = g[0].astype(F32) * factor
        g = (g.T if i == 2 else g)[None]
        m = 0.9 * m[...] + 0.1 * g
        v = 0.95 * v[...] + 0.05 * g * g
        w = w[...].astype(F32)
        w = w - 0.02 * (m * lax.rsqrt(v + 1e-8) + 0.1 * w)
        outs[i][...] = w.astype(BF16)
        outs[3 + i][...] = m
        outs[6 + i][...] = v


def adamw(factor, ws, ms, vs, gs, steps=16):
    specs = []
    for w in ws:
        layers, r, c = w.shape
        specs.append(pl.BlockSpec((1, r // steps, c), lambda l, f: (l, f, 0)))
    transposed = pl.BlockSpec((1, gs[2].shape[1], gs[2].shape[2] // steps), lambda l, f: (l, 0, f))
    ins, in_specs = [], []
    for i, (w, m, v, g, spec) in enumerate(zip(ws, ms, vs, gs, specs)):
        ins += [w, m, v, g]
        in_specs += [spec] * 3 + [transposed if i == 2 else spec]
    shapes = [jax.ShapeDtypeStruct(w.shape, t) for t in (BF16, F32, F32) for w in ws]
    return pl.pallas_call(
        adamw_kernel,
        grid=(ws[0].shape[0], steps),
        in_specs=[pl.BlockSpec(memory_space=pltpu.VMEM)] + in_specs,
        out_specs=specs * 3,
        out_shape=shapes,
        compiler_params=pltpu.CompilerParams(vmem_limit_bytes=VMEM_LIMIT),
        cost_estimate=pl.CostEstimate(flops=20 * 3 * ws[0].size, bytes_accessed=22 * 3 * ws[0].size, transcendentals=0),
        name="adamw",
    )(factor, *ins)


BLOCK, BLOCKS = 256, 16
WHOLE = 512
ORDERS = ((1, 8, 4, 2), (1, 4, 2, 8), (1, 2, 8, 4))
MATRICES = range(3)


def backward_kernel(tb, gathered, h_ref, dy_ref, a0t_ref, wg_ref, wu_ref, wd_ref, gate_ref, up_ref,
                    g0_ref, g1_ref, g2_ref, factor_ref,
                    a_ref, at_ref, dyt_ref, by_gate, by_up, hid_ref, dgate_ref, dup_ref,
                    keep0, keep1, keep2, keep3, send0, send1, send2, send3, recv0, recv1, recv2, recv3,
                    gbuf, squares, all_squares, rs_send, rs_recv, ag_send, ag_recv, out_sem, in_sem, sq_send, sq_recv):
    t = pl.program_id(0)
    tokens, d = a_ref.shape
    outs = (g0_ref, g1_ref, g2_ref)
    keep, send, recv = (keep0, keep1, keep2, keep3), (send0, send1, send2, send3), (recv0, recv1, recv2, recv3)
    me = lax.axis_index("dp")
    bits = {w: (me // w) % 2 for w in (1, 2, 4, 8)}
    partners = {w: me + w * (1 - 2 * bits[w]) for w in (1, 2, 4, 8)}
    layer = 1 - jnp.minimum(t // BLOCKS, 1)

    def rs_copy(i, m, slot):
        return pltpu.make_async_remote_copy(
            send[i].at[slot, m], recv[i].at[slot, m], rs_send.at[i, m, slot], rs_recv.at[i, m, slot],
            device_id={"dp": partners[ORDERS[m][i]]}, device_id_type=pl.DeviceIdType.MESH)

    def own_rows(m, phase):
        n = WHOLE >> (phase + 1)
        offset = sum(bits[ORDERS[m][q]] * (WHOLE >> (q + 1)) for q in range(phase + 1))
        return pl.ds(pl.multiple_of(offset, n), n)

    def ag_copy(j, m, b):
        part = gbuf.at[m, b % BLOCKS, own_rows(m, 3 - j), :]
        return pltpu.make_async_remote_copy(
            part, part, ag_send.at[j, m, b % 2], ag_recv.at[j, m, b % 2],
            device_id={"dp": partners[ORDERS[m][3 - j]]}, device_id_type=pl.DeviceIdType.MESH)

    def out_copy(m, b):
        columns = pl.ds(pl.multiple_of((b % BLOCKS) * BLOCK, BLOCK), BLOCK)
        return pltpu.make_async_copy(gbuf.at[m, b % BLOCKS], outs[m].at[1 - b // BLOCKS, :, columns], out_sem.at[m, b % 2])

    def half(bit, n):
        return pl.ds(pl.multiple_of(bit * n, n), n)

    @pl.when(t == 0)
    def _():
        first = pltpu.make_async_copy(a0t_ref, at_ref.at[0], in_sem)
        first.start()
        squares[...] = jnp.zeros_like(squares)
        for r in range(0, tokens, tb):
            rows = pl.ds(r, tb)
            wide = h_ref[rows, :].astype(F32)
            a = (wide * norm_scale(wide)).astype(BF16)
            a_ref[rows, :] = a
            at_ref[1, :, rows] = a.T
            dyt_ref[:, rows] = dy_ref[0, rows, :].T
            by_gate[rows, :] = jnp.zeros((tb, d), F32)
            by_up[rows, :] = jnp.zeros((tb, d), F32)
        first.wait()

    @pl.when(t < BLOCKS)
    def _():
        for r in range(0, tokens, tb):
            rows = pl.ds(r, tb)
            a = a_ref[rows, :]
            gate = dot(a, wg_ref[0], 1, 0)
            up = dot(a, wu_ref[0], 1, 0)
            dhid = dot(dy_ref[0, rows, :], wd_ref[0], 1, 1).astype(BF16).astype(F32)
            s = sigmoid(gate)
            silu = gate * s
            hid_ref[rows, :] = (silu * up).astype(BF16)
            dup = (dhid * silu).astype(BF16)
            dgate = (dhid * up * (s + silu * (1.0 - s))).astype(BF16)
            dup_ref[rows, :] = dup
            dgate_ref[rows, :] = dgate
            by_gate[rows, :] += dot(dgate, wg_ref[0], 1, 1)
            by_up[rows, :] += dot(dup, wu_ref[0], 1, 1)

    @pl.when(t == BLOCKS)
    def _():
        for r in range(0, tokens, tb):
            rows = pl.ds(r, tb)
            wide = h_ref[rows, :].astype(F32)
            scale = norm_scale(wide)
            da = (by_gate[rows, :].astype(BF16).astype(F32) + by_up[rows, :].astype(BF16).astype(F32)).astype(BF16).astype(F32)
            dn = scale * da - wide * (scale * scale * scale * jnp.mean(da * wide, -1, keepdims=True))
            dh = (dy_ref[0, rows, :].astype(F32) + dn.astype(BF16).astype(F32)).astype(BF16)
            a_ref[rows, :] = dh
            dyt_ref[:, rows] = dh.T

    @pl.when((t >= BLOCKS) & (t < 2 * BLOCKS))
    def _():
        for r in range(0, tokens, tb):
            rows = pl.ds(r, tb)
            gate, up = gate_ref[rows, :], up_ref[rows, :]
            dhid = dot(a_ref[rows, :], wd_ref[0], 1, 1).astype(BF16).astype(F32)
            s = sigmoid(gate)
            silu = gate * s
            hid_ref[rows, :] = (silu * up).astype(BF16)
            dup_ref[rows, :] = (dhid * silu).astype(BF16)
            dgate_ref[rows, :] = (dhid * up * (s + silu * (1.0 - s))).astype(BF16)

    def active(i):
        return (t >= i) & (t < i + (2 * BLOCKS if i < 5 else gathered))

    for i in (9, 8, 7, 6, 5):
        @pl.when(active(i))
        def _(i=i):
            for m in MATRICES:
                if i == 9:
                    out_copy(m, t - i).wait()
                else:
                    ag_copy(i - 5, m, t - i).wait()

    for i in (4, 3, 2, 1):
        @pl.when(active(i))
        def _(i=i):
            slot = (t - i) % 2
            for m in MATRICES:
                rs_copy(i - 1, m, slot).wait()
            for m in MATRICES:
                if i < 4:
                    n, bit = WHOLE >> (i + 1), bits[ORDERS[m][i]]
                    away, here = half(1 - bit, n), half(bit, n)
                    send[i][slot, m] = (keep[i - 1][m, away, :] + recv[i - 1][slot, m, away, :].astype(F32)).astype(BF16)
                    keep[i][m] = keep[i - 1][m, here, :] + recv[i - 1][slot, m, here, :].astype(F32)
                else:
                    g = (keep[3][m] + recv[3][slot, m].astype(F32)).astype(BF16)
                    gbuf[m, (t - i) % BLOCKS, own_rows(m, 3), :] = g
                    squares[...] += g.astype(F32) * g.astype(F32)

    for i in (8, 7, 6, 5, 4, 3, 2, 1):
        @pl.when(active(i) if i != 4 else (t >= 4) & (t < 4 + gathered))
        def _(i=i):
            for m in MATRICES:
                if i == 8:
                    out_copy(m, t - i).start()
                elif i >= 4:
                    ag_copy(i - 4, m, t - i).start()
                else:
                    rs_copy(i, m, (t - i) % 2).start()

    @pl.when(t < 2 * BLOCKS)
    def _():
        slot = t % 2
        for m, rhs in enumerate((dgate_ref, dup_ref, hid_ref)):
            bit = bits[ORDERS[m][0]]
            away, here = half(1 - bit, WHOLE // 2), half(bit, WHOLE // 2)
            left = (lambda rows: dyt_ref[rows, :]) if m == 2 else (lambda rows: at_ref[layer, rows, :])
            send[0][slot, m] = dot(left(away), rhs[...], 1, 0).astype(BF16)
            keep[0][m] = dot(left(here), rhs[...], 1, 0)
            rs_copy(0, m, slot).start()

    others = range(1, 16)

    def square_copy(k, row):
        return pltpu.make_async_remote_copy(
            all_squares.at[me], all_squares.at[row], sq_send.at[k], sq_recv.at[k],
            device_id={"dp": (me + k) % 16}, device_id_type=pl.DeviceIdType.MESH)

    @pl.when(t == 2 * BLOCKS + 4)
    def _():
        total = squares[0:8, :]
        for r in range(8, squares.shape[0], 8):
            total = total + squares[r : r + 8, :]
        all_squares[me] = total[:, :128] + total[:, 128:]
        for k in others:
            square_copy(k, me).start()

    @pl.when(t == pl.num_programs(0) - 1)
    def _():
        for k in others:
            copy = square_copy(k, (me + 16 - k) % 16)
            copy.wait_send()
            copy.wait_recv()
        total = all_squares[0]
        for k in others:
            total = total + all_squares[k]
        count = 2 * 3 * WHOLE * BLOCK * BLOCKS
        factor = jnp.minimum(1.0, 0.5 * lax.rsqrt(jnp.sum(total, keepdims=True) / count + 1e-30))
        factor_ref[...] = jnp.broadcast_to(factor, factor_ref.shape)


def backward(h, dy, a0t, ws, gate, up, gathered=2 * BLOCKS, tb=512):
    tokens, d = h.shape
    ff = gate.shape[1]
    assert (d, ff) == (WHOLE, BLOCK * BLOCKS)
    vmem = pl.BlockSpec(memory_space=pltpu.VMEM)
    anywhere = pl.BlockSpec(memory_space=pl.ANY)
    top_block = lambda t: (1, 0, jnp.minimum(t, BLOCKS - 1))
    low_block = lambda t: (0, jnp.minimum(jnp.maximum(t - BLOCKS, 0), BLOCKS - 1))

    def down_block(t):
        t = jnp.minimum(t, 2 * BLOCKS - 1)
        return (1 - t // BLOCKS, t % BLOCKS, 0)

    sizes = [WHOLE >> (i + 1) for i in range(4)]
    return pl.pallas_call(
        functools.partial(backward_kernel, tb, gathered),
        grid=(2 * BLOCKS + max(gathered - 2 * BLOCKS + 9, 6),),
        in_specs=[
            vmem, vmem, anywhere,
            pl.BlockSpec((1, d, BLOCK), top_block),
            pl.BlockSpec((1, d, BLOCK), top_block),
            pl.BlockSpec((1, BLOCK, d), down_block),
            pl.BlockSpec((tokens, BLOCK), low_block),
            pl.BlockSpec((tokens, BLOCK), low_block),
        ],
        out_specs=[anywhere] * 3 + [vmem],
        out_shape=[jax.ShapeDtypeStruct((2, WHOLE, ff), BF16)] * 3 + [jax.ShapeDtypeStruct((8, 128), F32)],
        scratch_shapes=[
            pltpu.VMEM((tokens, d), BF16),
            pltpu.VMEM((2, d, tokens), BF16),
            pltpu.VMEM((d, tokens), BF16),
            pltpu.VMEM((tokens, d), F32),
            pltpu.VMEM((tokens, d), F32),
            pltpu.VMEM((tokens, BLOCK), BF16),
            pltpu.VMEM((tokens, BLOCK), BF16),
            pltpu.VMEM((tokens, BLOCK), BF16),
            *[pltpu.VMEM((3, n, BLOCK), F32) for n in sizes],
            *[pltpu.VMEM((2, 3, n, BLOCK), BF16) for n in sizes],
            *[pltpu.VMEM((2, 3, n, BLOCK), BF16) for n in sizes],
            pltpu.VMEM((3, BLOCKS, WHOLE, BLOCK), BF16),
            pltpu.VMEM((sizes[3], BLOCK), F32),
            pltpu.VMEM((16, 8, 128), F32),
            pltpu.SemaphoreType.DMA((4, 3, 2)),
            pltpu.SemaphoreType.DMA((4, 3, 2)),
            pltpu.SemaphoreType.DMA((4, 3, 2)),
            pltpu.SemaphoreType.DMA((4, 3, 2)),
            pltpu.SemaphoreType.DMA((3, 2)),
            pltpu.SemaphoreType.DMA,
            pltpu.SemaphoreType.DMA((16,)),
            pltpu.SemaphoreType.DMA((16,)),
        ],
        compiler_params=pltpu.CompilerParams(vmem_limit_bytes=VMEM_LIMIT, has_side_effects=True),
        cost_estimate=pl.CostEstimate(flops=24 * tokens * d * ff, bytes_accessed=12 * tokens * ff, transcendentals=0),
        name="backward",
    )(h, dy, a0t, *ws, gate, up)


def solution(mesh):
    def step(x, dy, *arrays):
        ws, ms, vs = (arrays[i : i + 3] for i in (0, 3, 6))
        gate, up, h, at = forward(x, *ws)
        *gs, factor = backward(h, dy, at, ws, gate, up)
        return tuple(adamw(factor, ws, ms, vs, gs))

    return jax.shard_map(
        step,
        mesh=mesh,
        in_specs=(P(("rep", "dp"), None, None),) * 2 + (P(None, None, None),) * 9,
        out_specs=(P("rep", None, None),) * 9,
        check_vma=False,
    )
```

```python
import functools
import jax
import jax.numpy as jnp
from jax import lax
from jax.experimental import pallas as pl
from jax.experimental.pallas import tpu as pltpu
from jax.sharding import PartitionSpec as P

F32, BF16 = jnp.float32, jnp.bfloat16
VMEM_LIMIT = 67_000_000


def dot(a, b, da, db):
    return lax.dot_general(a, b, (((da,), (db,)), ((), ())), preferred_element_type=F32)


def norm_scale(wide):
    return lax.rsqrt(jnp.mean(wide * wide, -1, keepdims=True) + 1e-6)


def sigmoid(g):
    return 1.0 / (1.0 + jnp.exp(-g))


def interleave(n, first, second, third):
    for r in range(n + 2):
        if r < n:
            first(r)
        if 0 <= r - 2:
            third(r - 2)
        if 0 <= r - 1 < n:
            second(r - 1)


def forward_kernel(tb, x_ref, wg_ref, wu_ref, wd_ref, gate_ref, up_ref, h_ref, at_ref, a_ref, acc_ref, hid_ref):
    f, last = pl.program_id(0), pl.num_programs(0) - 1
    tokens = acc_ref.shape[0]

    @pl.when(f == 0)
    def _():
        for t in range(0, tokens, tb):
            rows = pl.ds(t, tb)
            wide = x_ref[0, rows, :].astype(F32)
            a = (wide * norm_scale(wide)).astype(BF16)
            a_ref[rows, :] = a
            at_ref[:, rows] = a.T
            acc_ref[rows, :] = jnp.zeros((tb, acc_ref.shape[1]), F32)

    def project(r):
        rows = pl.ds(r * tb, tb)
        gate_ref[rows, :] = dot(a_ref[rows, :], wg_ref[0], 1, 0)
        up_ref[rows, :] = dot(a_ref[rows, :], wu_ref[0], 1, 0)

    def product(r):
        rows = pl.ds(r * tb, tb)
        gate = gate_ref[rows, :]
        hid_ref[rows, :] = (gate * sigmoid(gate) * up_ref[rows, :]).astype(BF16)

    def down(r):
        rows = pl.ds(r * tb, tb)
        acc_ref[rows, :] += dot(hid_ref[rows, :], wd_ref[0], 1, 0)

    interleave(tokens // tb, project, product, down)

    @pl.when(f == last)
    def _():
        for t in range(0, tokens, tb):
            rows = pl.ds(t, tb)
            h_ref[rows, :] = (x_ref[0, rows, :].astype(F32) + acc_ref[rows, :].astype(BF16).astype(F32)).astype(BF16)


def forward(x, wg, wu, wd, fb=256, tb=512):
    _, tokens, d = x.shape
    ff = wg.shape[2]
    whole = lambda *s: pl.BlockSpec(s, lambda f: (0,) * len(s))
    return pl.pallas_call(
        functools.partial(forward_kernel, tb),
        grid=(ff // fb,),
        in_specs=[
            whole(1, tokens, d),
            pl.BlockSpec((1, d, fb), lambda f: (0, 0, f)),
            pl.BlockSpec((1, d, fb), lambda f: (0, 0, f)),
            pl.BlockSpec((1, fb, d), lambda f: (0, f, 0)),
        ],
        out_specs=[
            pl.BlockSpec((tokens, fb), lambda f: (0, f)),
            pl.BlockSpec((tokens, fb), lambda f: (0, f)),
            whole(tokens, d),
            whole(d, tokens),
        ],
        out_shape=[
            jax.ShapeDtypeStruct((tokens, ff), F32),
            jax.ShapeDtypeStruct((tokens, ff), F32),
            jax.ShapeDtypeStruct((tokens, d), BF16),
            jax.ShapeDtypeStruct((d, tokens), BF16),
        ],
        scratch_shapes=[pltpu.VMEM((tokens, d), BF16), pltpu.VMEM((tokens, d), F32), pltpu.VMEM((tokens, fb), BF16)],
        compiler_params=pltpu.CompilerParams(vmem_limit_bytes=VMEM_LIMIT),
        cost_estimate=pl.CostEstimate(flops=6 * tokens * d * ff, bytes_accessed=9 * tokens * ff, transcendentals=0),
        name="forward",
    )(x, wg, wu, wd)


def adamw_kernel(factor_ref, *refs):
    ins, outs = refs[:12], refs[12:]
    factor = factor_ref[0:1, 0:1]
    for i in range(3):
        w, m, v, g = (ins[4 * i + j] for j in range(4))
        g = g[0].astype(F32) * factor
        g = (g.T if i == 2 else g)[None]
        m = 0.9 * m[...] + 0.1 * g
        v = 0.95 * v[...] + 0.05 * g * g
        w = w[...].astype(F32)
        w = w - 0.02 * (m * lax.rsqrt(v + 1e-8) + 0.1 * w)
        outs[i][...] = w.astype(BF16)
        outs[3 + i][...] = m
        outs[6 + i][...] = v


def adamw(factor, ws, ms, vs, gs, steps=8):
    specs = []
    for w in ws:
        layers, r, c = w.shape
        specs.append(pl.BlockSpec((1, r // steps, c), lambda l, f: (l, f, 0)))
    transposed = pl.BlockSpec((1, gs[2].shape[1], gs[2].shape[2] // steps), lambda l, f: (l, 0, f))
    ins, in_specs = [], []
    for i, (w, m, v, g, spec) in enumerate(zip(ws, ms, vs, gs, specs)):
        ins += [w, m, v, g]
        in_specs += [spec] * 3 + [transposed if i == 2 else spec]
    shapes = [jax.ShapeDtypeStruct(w.shape, t) for t in (BF16, F32, F32) for w in ws]
    return pl.pallas_call(
        adamw_kernel,
        grid=(ws[0].shape[0], steps),
        in_specs=[pl.BlockSpec(memory_space=pltpu.VMEM)] + in_specs,
        out_specs=specs * 3,
        out_shape=shapes,
        compiler_params=pltpu.CompilerParams(vmem_limit_bytes=VMEM_LIMIT),
        cost_estimate=pl.CostEstimate(flops=20 * 3 * ws[0].size, bytes_accessed=22 * 3 * ws[0].size, transcendentals=0),
        name="adamw",
    )(factor, *ins)


BLOCK, BLOCKS = 256, 16
WHOLE = 512
ORDERS = ((1, 8, 4, 2), (1, 4, 2, 8), (1, 2, 8, 4))
MATRICES = range(3)


def backward_kernel(tb, h_ref, dy_ref, a0t_ref, wg_ref, wu_ref, wd_ref, gate_ref, up_ref,
                    g0_ref, g1_ref, g2_ref, factor_ref,
                    a_ref, at_ref, dyt_ref, by_gate, by_up, hid_ref, dgate_ref, dup_ref, gate_buf, up_buf, dhid_buf,
                    own_term, keep1, keep2, keep3, send0, send1, send2, send3, recv0, recv1, recv2, recv3,
                    gbuf, squares, all_squares, rs_send, rs_recv, ag_send, ag_recv, out_sem, in_sem, sq_send, sq_recv):
    t = pl.program_id(0)
    tokens, d = a_ref.shape
    outs = (g0_ref, g1_ref, g2_ref)
    keep, send, recv = (None, keep1, keep2, keep3), (send0, send1, send2, send3), (recv0, recv1, recv2, recv3)
    me = lax.axis_index("dp")
    bits = {w: (me // w) % 2 for w in (1, 2, 4, 8)}
    partners = {w: me + w * (1 - 2 * bits[w]) for w in (1, 2, 4, 8)}

    def rs_copy(i, m, slot):
        return pltpu.make_async_remote_copy(
            send[i].at[slot, m], recv[i].at[slot, m], rs_send.at[i, m, slot], rs_recv.at[i, m, slot],
            device_id={"dp": partners[ORDERS[m][i]]}, device_id_type=pl.DeviceIdType.MESH)

    def own_rows(m, phase):
        n = WHOLE >> (phase + 1)
        offset = sum(bits[ORDERS[m][q]] * (WHOLE >> (q + 1)) for q in range(phase + 1))
        return pl.ds(pl.multiple_of(offset, n), n)

    def ag_copy(j, m, b):
        part = gbuf.at[m, b % BLOCKS, own_rows(m, 3 - j), :]
        return pltpu.make_async_remote_copy(
            part, part, ag_send.at[j, m, b % 2], ag_recv.at[j, m, b % 2],
            device_id={"dp": partners[ORDERS[m][3 - j]]}, device_id_type=pl.DeviceIdType.MESH)

    def out_copy(m, b):
        columns = pl.ds(pl.multiple_of((b % BLOCKS) * BLOCK, BLOCK), BLOCK)
        return pltpu.make_async_copy(gbuf.at[m, b % BLOCKS], outs[m].at[1 - b // BLOCKS, :, columns], out_sem.at[m, b % 2])

    def half(bit, n):
        return pl.ds(pl.multiple_of(bit * n, n), n)

    @pl.when(t == 0)
    def _():
        first = pltpu.make_async_copy(a0t_ref, at_ref.at[0], in_sem)
        first.start()
        squares[...] = jnp.zeros_like(squares)
        for r in range(0, tokens, tb):
            rows = pl.ds(r, tb)
            wide = h_ref[rows, :].astype(F32)
            a = (wide * norm_scale(wide)).astype(BF16)
            a_ref[rows, :] = a
            at_ref[1, :, rows] = a.T
            dyt_ref[:, rows] = dy_ref[0, rows, :].T
            by_gate[rows, :] = jnp.zeros((tb, d), F32)
            by_up[rows, :] = jnp.zeros((tb, d), F32)
        first.wait()

    @pl.when(t == BLOCKS)
    def _():
        for r in range(0, tokens, tb):
            rows = pl.ds(r, tb)
            wide = h_ref[rows, :].astype(F32)
            scale = norm_scale(wide)
            da = (by_gate[rows, :].astype(BF16).astype(F32) + by_up[rows, :].astype(BF16).astype(F32)).astype(BF16).astype(F32)
            dn = scale * da - wide * (scale * scale * scale * jnp.mean(da * wide, -1, keepdims=True))
            dh = (dy_ref[0, rows, :].astype(F32) + dn.astype(BF16).astype(F32)).astype(BF16)
            a_ref[rows, :] = dh
            dyt_ref[:, rows] = dh.T

    def wait_and_add(i):
        b = t - i
        slot = b % 2
        for m in MATRICES:
            if 2 <= i <= 5:
                rs_copy(i - 2, m, slot).wait()
            elif 6 <= i <= 9:
                ag_copy(i - 6, m, b).wait()
            elif i == 10:
                out_copy(m, b).wait()
        for m in MATRICES:
            if i == 1:
                send[0][slot, m] = own_term[slot, m, half(1 - bits[ORDERS[m][0]], WHOLE // 2), :].astype(BF16)
            elif i < 5:
                n, bit = WHOLE >> i, bits[ORDERS[m][i - 1]]
                away, here = half(1 - bit, n), half(bit, n)
                if i == 2:
                    base = bits[ORDERS[m][0]] * 2
                    mine = own_term[slot, m, half(base + 1 - bit, n), :], own_term[slot, m, half(base + bit, n), :]
                else:
                    mine = keep[i - 2][m, away, :], keep[i - 2][m, here, :]
                send[i - 1][slot, m] = (mine[0] + recv[i - 2][slot, m, away, :].astype(F32)).astype(BF16)
                keep[i - 1][m] = mine[1] + recv[i - 2][slot, m, here, :].astype(F32)
            elif i == 5:
                g = (keep[3][m] + recv[3][slot, m].astype(F32)).astype(BF16)
                gbuf[m, b % BLOCKS, own_rows(m, 3), :] = g
                squares[...] += g.astype(F32) * g.astype(F32)

    def start(i):
        for m in MATRICES:
            if i <= 4:
                rs_copy(i - 1, m, (t - i) % 2).start()
            elif i <= 8:
                ag_copy(i - 5, m, t - i).start()
            elif i == 9:
                out_copy(m, t - i).start()

    steady = (t >= 10) & (t < 2 * BLOCKS + 1)

    @pl.when(steady)
    def _():
        for i in range(10, 0, -1):
            wait_and_add(i)
        for i in range(9, 0, -1):
            start(i)

    @pl.when(jnp.logical_not(steady))
    def _():
        for act in (wait_and_add, start):
            for i in range(10, 0, -1):
                pl.when((t >= i) & (t < i + 2 * BLOCKS))(functools.partial(act, i))

    def elementwise(r, gate, up, dhid):
        rows = pl.ds(r * tb, tb)
        dhid = dhid.astype(BF16).astype(F32)
        s = sigmoid(gate)
        silu = gate * s
        hid_ref[rows, :] = (silu * up).astype(BF16)
        dup_ref[rows, :] = (dhid * silu).astype(BF16)
        dgate_ref[rows, :] = (dhid * up * (s + silu * (1.0 - s))).astype(BF16)

    def weight_terms(r, which):
        rows = pl.ds(r * tb, tb)
        for m, rhs in enumerate((dgate_ref, dup_ref, hid_ref)):
            term = dot(dyt_ref[:, rows] if m == 2 else at_ref[which, :, rows], rhs[rows, :], 1, 0)
            own_term[t % 2, m] = term if r == 0 else own_term[t % 2, m] + term

    @pl.when(t < BLOCKS)
    def _():
        def first(r):
            rows = pl.ds(r * tb, tb)
            gate_buf[r % 2] = dot(a_ref[rows, :], wg_ref[0], 1, 0)
            up_buf[r % 2] = dot(a_ref[rows, :], wu_ref[0], 1, 0)
            dhid_buf[r % 2] = dot(dy_ref[0, rows, :], wd_ref[0], 1, 1)

        def second(r):
            elementwise(r, gate_buf[r % 2], up_buf[r % 2], dhid_buf[r % 2])

        def third(r):
            rows = pl.ds(r * tb, tb)
            by_gate[rows, :] += dot(dgate_ref[rows, :], wg_ref[0], 1, 1)
            by_up[rows, :] += dot(dup_ref[rows, :], wu_ref[0], 1, 1)
            weight_terms(r, 1)

        interleave(tokens // tb, first, second, third)

    @pl.when((t >= BLOCKS) & (t < 2 * BLOCKS))
    def _():
        def first(r):
            dhid_buf[r % 2] = dot(a_ref[pl.ds(r * tb, tb), :], wd_ref[0], 1, 1)

        def second(r):
            rows = pl.ds(r * tb, tb)
            elementwise(r, gate_ref[rows, :], up_ref[rows, :], dhid_buf[r % 2])

        interleave(tokens // tb, first, second, lambda r: weight_terms(r, 0))

    others = range(1, 16)

    def square_copy(k, row):
        return pltpu.make_async_remote_copy(
            all_squares.at[me], all_squares.at[row], sq_send.at[k], sq_recv.at[k],
            device_id={"dp": (me + k) % 16}, device_id_type=pl.DeviceIdType.MESH)

    @pl.when(t == 2 * BLOCKS + 5)
    def _():
        total = squares[0:8, :]
        for r in range(8, squares.shape[0], 8):
            total = total + squares[r : r + 8, :]
        all_squares[me] = total[:, :128] + total[:, 128:]
        for k in others:
            square_copy(k, me).start()

    @pl.when(t == pl.num_programs(0) - 1)
    def _():
        for k in others:
            copy = square_copy(k, (me + 16 - k) % 16)
            copy.wait_send()
            copy.wait_recv()
        total = all_squares[0]
        for k in others:
            total = total + all_squares[k]
        count = 2 * 3 * WHOLE * BLOCK * BLOCKS
        factor = jnp.minimum(1.0, 0.5 * lax.rsqrt(jnp.sum(total, keepdims=True) / count + 1e-30))
        factor_ref[...] = jnp.broadcast_to(factor, factor_ref.shape)


def backward(h, dy, a0t, ws, gate, up, tb=512):
    tokens, d = h.shape
    ff = gate.shape[1]
    assert (d, ff) == (WHOLE, BLOCK * BLOCKS)
    vmem = pl.BlockSpec(memory_space=pltpu.VMEM)
    anywhere = pl.BlockSpec(memory_space=pl.ANY)
    top_block = lambda t: (1, 0, jnp.minimum(t, BLOCKS - 1))
    low_block = lambda t: (0, jnp.minimum(jnp.maximum(t - BLOCKS, 0), BLOCKS - 1))

    def down_block(t):
        t = jnp.minimum(t, 2 * BLOCKS - 1)
        return (1 - t // BLOCKS, t % BLOCKS, 0)

    sizes = [WHOLE >> (i + 1) for i in range(4)]
    return pl.pallas_call(
        functools.partial(backward_kernel, tb),
        grid=(2 * BLOCKS + 10,),
        in_specs=[
            vmem, vmem, anywhere,
            pl.BlockSpec((1, d, BLOCK), top_block),
            pl.BlockSpec((1, d, BLOCK), top_block),
            pl.BlockSpec((1, BLOCK, d), down_block),
            pl.BlockSpec((tokens, BLOCK), low_block),
            pl.BlockSpec((tokens, BLOCK), low_block),
        ],
        out_specs=[anywhere] * 3 + [vmem],
        out_shape=[jax.ShapeDtypeStruct((2, WHOLE, ff), BF16)] * 3 + [jax.ShapeDtypeStruct((8, 128), F32)],
        scratch_shapes=[
            pltpu.VMEM((tokens, d), BF16),
            pltpu.VMEM((2, d, tokens), BF16),
            pltpu.VMEM((d, tokens), BF16),
            pltpu.VMEM((tokens, d), F32),
            pltpu.VMEM((tokens, d), F32),
            pltpu.VMEM((tokens, BLOCK), BF16),
            pltpu.VMEM((tokens, BLOCK), BF16),
            pltpu.VMEM((tokens, BLOCK), BF16),
            *[pltpu.VMEM((2, tb, BLOCK), F32)] * 3,
            pltpu.VMEM((2, 3, WHOLE, BLOCK), F32),
            *[pltpu.VMEM((3, n, BLOCK), F32) for n in sizes[1:]],
            *[pltpu.VMEM((2, 3, n, BLOCK), BF16) for n in sizes],
            *[pltpu.VMEM((2, 3, n, BLOCK), BF16) for n in sizes],
            pltpu.VMEM((3, BLOCKS, WHOLE, BLOCK), BF16),
            pltpu.VMEM((sizes[3], BLOCK), F32),
            pltpu.VMEM((16, 8, 128), F32),
            pltpu.SemaphoreType.DMA((4, 3, 2)),
            pltpu.SemaphoreType.DMA((4, 3, 2)),
            pltpu.SemaphoreType.DMA((4, 3, 2)),
            pltpu.SemaphoreType.DMA((4, 3, 2)),
            pltpu.SemaphoreType.DMA((3, 2)),
            pltpu.SemaphoreType.DMA,
            pltpu.SemaphoreType.DMA((16,)),
            pltpu.SemaphoreType.DMA((16,)),
        ],
        compiler_params=pltpu.CompilerParams(vmem_limit_bytes=VMEM_LIMIT, has_side_effects=True),
        cost_estimate=pl.CostEstimate(flops=24 * tokens * d * ff, bytes_accessed=12 * tokens * ff, transcendentals=0),
        name="backward",
    )(h, dy, a0t, *ws, gate, up)


def solution(mesh):
    def step(x, dy, *arrays):
        ws, ms, vs = (arrays[i : i + 3] for i in (0, 3, 6))
        gate, up, h, at = forward(x, *ws)
        *gs, factor = backward(h, dy, at, ws, gate, up)
        return tuple(adamw(factor, ws, ms, vs, gs))

    return jax.shard_map(
        step,
        mesh=mesh,
        in_specs=(P(("rep", "dp"), None, None),) * 2 + (P(None, None, None),) * 9,
        out_specs=(P("rep", None, None),) * 9,
        check_vma=False,
    )
```

```python
import functools
import jax
import jax.numpy as jnp
from jax import lax
from jax.experimental import pallas as pl
from jax.experimental.pallas import tpu as pltpu
from jax.sharding import PartitionSpec as P

F32, BF16 = jnp.float32, jnp.bfloat16
VMEM_LIMIT = 67_000_000


def dot(a, b, da, db):
    return lax.dot_general(a, b, (((da,), (db,)), ((), ())), preferred_element_type=F32)


def norm_scale(wide):
    return lax.rsqrt(jnp.mean(wide * wide, -1, keepdims=True) + 1e-6)


def sigmoid(g):
    return 1.0 / (1.0 + jnp.exp(-g))


def interleave(n, first, second, third):
    for r in range(n + 2):
        if r < n:
            first(r)
        if 0 <= r - 2:
            third(r - 2)
        if 0 <= r - 1 < n:
            second(r - 1)


def forward_kernel(tb, x_ref, wg_ref, wu_ref, wd_ref, gate_ref, up_ref, h_ref, at_ref, a_ref, acc_ref, hid_ref):
    f, last = pl.program_id(0), pl.num_programs(0) - 1
    tokens = acc_ref.shape[0]

    @pl.when(f == 0)
    def _():
        for t in range(0, tokens, 128):
            rows = pl.ds(t, 128)
            wide = x_ref[0, rows, :].astype(F32)
            a = (wide * norm_scale(wide)).astype(BF16)
            a_ref[rows, :] = a
            at_ref[:, rows] = a.T
            acc_ref[rows, :] = jnp.zeros((128, acc_ref.shape[1]), F32)

    def project(r):
        rows = pl.ds(r * tb, tb)
        gate_ref[rows, :] = dot(a_ref[rows, :], wg_ref[0], 1, 0)
        up_ref[rows, :] = dot(a_ref[rows, :], wu_ref[0], 1, 0)

    def product(r):
        rows = pl.ds(r * tb, tb)
        gate = gate_ref[rows, :]
        hid_ref[rows, :] = (gate * sigmoid(gate) * up_ref[rows, :]).astype(BF16)

    def down(r):
        rows = pl.ds(r * tb, tb)
        acc_ref[rows, :] += dot(hid_ref[rows, :], wd_ref[0], 1, 0)

    interleave(tokens // tb, project, product, down)

    @pl.when(f == last)
    def _():
        for t in range(0, tokens, tb):
            rows = pl.ds(t, tb)
            h_ref[rows, :] = (x_ref[0, rows, :].astype(F32) + acc_ref[rows, :].astype(BF16).astype(F32)).astype(BF16)


def forward(x, wg, wu, wd, fb=256, tb=512):
    _, tokens, d = x.shape
    ff = wg.shape[2]
    whole = lambda *s: pl.BlockSpec(s, lambda f: (0,) * len(s))
    return pl.pallas_call(
        functools.partial(forward_kernel, tb),
        grid=(ff // fb,),
        in_specs=[
            whole(1, tokens, d),
            pl.BlockSpec((1, d, fb), lambda f: (0, 0, f)),
            pl.BlockSpec((1, d, fb), lambda f: (0, 0, f)),
            pl.BlockSpec((1, fb, d), lambda f: (0, f, 0)),
        ],
        out_specs=[
            pl.BlockSpec((tokens, fb), lambda f: (0, f)),
            pl.BlockSpec((tokens, fb), lambda f: (0, f)),
            whole(tokens, d),
            whole(d, tokens),
        ],
        out_shape=[
            jax.ShapeDtypeStruct((tokens, ff), F32),
            jax.ShapeDtypeStruct((tokens, ff), F32),
            jax.ShapeDtypeStruct((tokens, d), BF16),
            jax.ShapeDtypeStruct((d, tokens), BF16),
        ],
        scratch_shapes=[pltpu.VMEM((tokens, d), BF16), pltpu.VMEM((tokens, d), F32), pltpu.VMEM((tokens, fb), BF16)],
        compiler_params=pltpu.CompilerParams(vmem_limit_bytes=VMEM_LIMIT),
        cost_estimate=pl.CostEstimate(flops=6 * tokens * d * ff, bytes_accessed=9 * tokens * ff, transcendentals=0),
        name="forward",
    )(x, wg, wu, wd)


def adamw(w, m, v, g):
    m = 0.9 * m + 0.1 * g
    v = 0.95 * v + 0.05 * g * g
    w = w.astype(F32)
    return (w - 0.02 * (m * lax.rsqrt(v + 1e-8) + 0.1 * w)).astype(BF16), m, v


def top_adamw_kernel(factor_ref, *refs):
    ins, outs = refs[:12], refs[12:]
    for i in range(3):
        w, m, v, g = ins[4 * i : 4 * i + 4]
        g = g[...].astype(F32) * factor_ref[0:1, 0:1]
        for out, new in zip(outs[i::3], adamw(w[0], m[0], v[0], g.T if i == 2 else g)):
            out[0] = new


def low_adamw_kernel(me_ref, factor_ref, *refs):
    ins, outs, scratch = refs[:21], refs[30:39], refs[39:]
    me = me_ref[0]
    for i in range(3):
        w, m, v = ins[7 * i : 7 * i + 3]
        own, across = me % 2, (me // ORDERS[i][1]) % 2
        for k, piece in enumerate(ins[7 * i + 3 : 7 * i + 7]):
            core, chip = (1 - own if k & 1 else own), (1 - across if k & 2 else across)
            rows = pl.ds(pl.multiple_of(core * (WHOLE // 2) + chip * (WHOLE // 4), WHOLE // 4), WHOLE // 4)
            for c in range(piece.shape[0]):
                scratch[i][rows, c * BLOCK : (c + 1) * BLOCK] = piece[c]
        g = scratch[i][...].astype(F32) * factor_ref[0:1, 0:1]
        for out, new in zip(outs[i::3], adamw(w[0], m[0], v[0], g.T if i == 2 else g)):
            out[0] = new


def adamw_parts(layer, steps, ws):
    wide = ws[0].shape[2] // steps
    low = pl.BlockSpec((1, ws[0].shape[1], wide), lambda f: (layer, 0, f))
    down = pl.BlockSpec((1, wide, ws[2].shape[2]), lambda f: (layer, f, 0))
    shapes = [jax.ShapeDtypeStruct(w.shape, t) for t in (BF16, F32, F32) for w in ws]
    return wide, [low, low, down], shapes


def top_adamw(factor, ws, ms, vs, gs, steps=8):
    wide, specs, shapes = adamw_parts(1, steps, ws)
    ins, in_specs = [], []
    for w, m, v, g, spec in zip(ws, ms, vs, gs, specs):
        ins += [w, m, v, g]
        in_specs += [spec] * 3 + [pl.BlockSpec((WHOLE, wide), lambda f: (0, f))]
    return pl.pallas_call(
        top_adamw_kernel,
        grid=(steps,),
        in_specs=[pl.BlockSpec(memory_space=pltpu.VMEM)] + in_specs,
        out_specs=specs * 3,
        out_shape=shapes,
        compiler_params=pltpu.CompilerParams(vmem_limit_bytes=VMEM_LIMIT),
        cost_estimate=pl.CostEstimate(flops=100_000_000_000, bytes_accessed=140_000_000, transcendentals=0),
        name="top_adamw",
    )(factor, *ins)


def low_adamw(me, factor, ws, ms, vs, pieces, partly, steps=8):
    wide, specs, shapes = adamw_parts(0, steps, ws)
    part = pl.BlockSpec((wide // BLOCK, WHOLE // 4, BLOCK), lambda f: (f, 0, 0))
    ins, in_specs = [], []
    for w, m, v, four, spec in zip(ws, ms, vs, pieces, specs):
        ins += [w, m, v, *four]
        in_specs += [spec] * 3 + [part] * 4
    return pl.pallas_call(
        low_adamw_kernel,
        grid=(steps,),
        in_specs=[pl.BlockSpec(memory_space=pltpu.SMEM), pl.BlockSpec(memory_space=pltpu.VMEM)] + in_specs + [pl.BlockSpec(memory_space=pl.ANY)] * 9,
        out_specs=specs * 3,
        out_shape=shapes,
        scratch_shapes=[pltpu.VMEM((WHOLE, wide), BF16)] * 3,
        input_output_aliases={23 + i: i for i in range(9)},
        compiler_params=pltpu.CompilerParams(vmem_limit_bytes=VMEM_LIMIT),
        cost_estimate=pl.CostEstimate(flops=100_000_000_000, bytes_accessed=140_000_000, transcendentals=0),
        name="low_adamw",
    )(me, factor, *ins, *partly)


BLOCK, BLOCKS = 256, 16
WHOLE = 512
SLOTS = 4
AT = (0, 1, 2, 3, 4, 5, 7, 9, 11, 13, 14)
ORDERS = ((1, 8, 4, 2), (1, 4, 2, 8), (1, 2, 8, 4))
MATRICES = range(3)


def backward_kernel(tb, h_ref, dy_ref, a0t_ref, wg_ref, wu_ref, wd_ref, gate_ref, up_ref,
                    g0_ref, g1_ref, g2_ref, q0_ref, q1_ref, q2_ref, factor_ref,
                    a_ref, at_ref, dyt_ref, by_gate, by_up, hid_ref, dgate_ref, dup_ref, gate_buf, up_buf, dhid_buf,
                    own_term, keep1, keep2, keep3, send0, send1, send2, send3, recv0, recv1, recv2, recv3,
                    gbuf, squares, all_squares, rs_send, rs_recv, ag_send, ag_recv, out_sem, in_sem, sq_send, sq_recv):
    t = pl.program_id(0)
    tokens, d = a_ref.shape
    outs, quarters = (g0_ref, g1_ref, g2_ref), (q0_ref, q1_ref, q2_ref)
    keep, send, recv = (None, keep1, keep2, keep3), (send0, send1, send2, send3), (recv0, recv1, recv2, recv3)
    me = lax.axis_index("dp")
    bits = {w: (me // w) % 2 for w in (1, 2, 4, 8)}
    partners = {w: me + w * (1 - 2 * bits[w]) for w in (1, 2, 4, 8)}

    def rs_copy(i, m, slot):
        return pltpu.make_async_remote_copy(
            send[i].at[slot, m], recv[i].at[slot, m], rs_send.at[i, m, slot], rs_recv.at[i, m, slot],
            device_id={"dp": partners[ORDERS[m][i]]}, device_id_type=pl.DeviceIdType.MESH)

    def own_rows(m, phase):
        n = WHOLE >> (phase + 1)
        offset = sum(bits[ORDERS[m][q]] * (WHOLE >> (q + 1)) for q in range(phase + 1))
        return pl.ds(pl.multiple_of(offset, n), n)

    def ag_copy(j, m, b):
        part = gbuf.at[m, b % BLOCKS, own_rows(m, 3 - j), :]
        return pltpu.make_async_remote_copy(
            part, part, ag_send.at[j, m, b % SLOTS], ag_recv.at[j, m, b % SLOTS],
            device_id={"dp": partners[ORDERS[m][3 - j]]}, device_id_type=pl.DeviceIdType.MESH)

    def out_copy(m, b):
        columns = pl.ds(pl.multiple_of((b % BLOCKS) * BLOCK, BLOCK), BLOCK)
        return pltpu.make_async_copy(gbuf.at[m, b % BLOCKS], outs[m].at[:, columns], out_sem.at[m, b % 2])

    def quarter_copy(m, b):
        return pltpu.make_async_copy(gbuf.at[m, b % BLOCKS, own_rows(m, 1), :], quarters[m].at[b % BLOCKS], out_sem.at[m, b % 2])

    def half(bit, n):
        return pl.ds(pl.multiple_of(bit * n, n), n)

    @pl.when(t == 0)
    def _():
        first = pltpu.make_async_copy(a0t_ref, at_ref.at[0], in_sem)
        first.start()
        squares[...] = jnp.zeros_like(squares)
        for r in range(0, tokens, 128):
            rows = pl.ds(r, 128)
            wide = h_ref[rows, :].astype(F32)
            a = (wide * norm_scale(wide)).astype(BF16)
            a_ref[rows, :] = a
            at_ref[1, :, rows] = a.T
            dyt_ref[:, rows] = dy_ref[0, rows, :].T
            by_gate[rows, :] = jnp.zeros((128, d), F32)
            by_up[rows, :] = jnp.zeros((128, d), F32)
        first.wait()

    @pl.when(t == BLOCKS)
    def _():
        for r in range(0, tokens, 128):
            rows = pl.ds(r, 128)
            wide = h_ref[rows, :].astype(F32)
            scale = norm_scale(wide)
            da = (by_gate[rows, :].astype(BF16).astype(F32) + by_up[rows, :].astype(BF16).astype(F32)).astype(BF16).astype(F32)
            dn = scale * da - wide * (scale * scale * scale * jnp.mean(da * wide, -1, keepdims=True))
            dh = (dy_ref[0, rows, :].astype(F32) + dn.astype(BF16).astype(F32)).astype(BF16)
            a_ref[rows, :] = dh
            dyt_ref[:, rows] = dh.T

    def reduce_stage(i):
        b = t - AT[i]
        slot, pair = b % SLOTS, b % 2
        for m in MATRICES:
            if i > 1:
                rs_copy(i - 2, m, slot).wait()
        for m in MATRICES:
            if i == 1:
                send[0][slot, m] = own_term[pair, m, half(1 - bits[ORDERS[m][0]], WHOLE // 2), :].astype(BF16)
            elif i < 5:
                n, bit = WHOLE >> i, bits[ORDERS[m][i - 1]]
                away, here = half(1 - bit, n), half(bit, n)
                if i == 2:
                    base = bits[ORDERS[m][0]] * 2
                    mine = own_term[pair, m, half(base + 1 - bit, n), :], own_term[pair, m, half(base + bit, n), :]
                else:
                    mine = keep[i - 2][pair, m, away, :], keep[i - 2][pair, m, here, :]
                send[i - 1][slot, m] = (mine[0] + recv[i - 2][slot, m, away, :].astype(F32)).astype(BF16)
                keep[i - 1][pair, m] = mine[1] + recv[i - 2][slot, m, here, :].astype(F32)
            elif i == 5:
                g = (keep[3][pair, m] + recv[3][slot, m].astype(F32)).astype(BF16)
                gbuf[m, b % BLOCKS, own_rows(m, 3), :] = g
                squares[...] += g.astype(F32) * g.astype(F32)

    def reduce_start(i):
        for m in MATRICES:
            rs_copy(i - 1, m, (t - AT[i]) % SLOTS).start()

    def each(copy, wait):
        def act(b):
            for m in MATRICES:
                copy(m, b).wait() if wait else copy(m, b).start()
        return act

    gathers = [functools.partial(ag_copy, j) for j in range(4)]

    def when_active(i, first, count, act):
        b = t - AT[i]
        pl.when((b >= first) & (b < first + count))(functools.partial(act, b))

    when_active(10, 0, BLOCKS, each(out_copy, True))
    when_active(9, 0, BLOCKS, each(gathers[3], True))
    when_active(8, 0, BLOCKS, each(gathers[2], True))
    when_active(8, BLOCKS, BLOCKS, each(quarter_copy, True))
    when_active(7, 0, 2 * BLOCKS, each(gathers[1], True))
    when_active(6, 0, 2 * BLOCKS, each(gathers[0], True))
    steady = (t >= AT[5]) & (t < 2 * BLOCKS + AT[1])

    @pl.when(steady)
    def _():
        for i in range(5, 0, -1):
            reduce_stage(i)
        for i in range(1, 5):
            reduce_start(i)

    @pl.when(jnp.logical_not(steady))
    def _():
        for act, stages in ((reduce_stage, range(5, 0, -1)), (reduce_start, range(1, 5))):
            for i in stages:
                pl.when((t >= AT[i]) & (t < AT[i] + 2 * BLOCKS))(functools.partial(act, i))

    when_active(5, 0, 2 * BLOCKS, each(gathers[0], False))
    when_active(6, 0, 2 * BLOCKS, each(gathers[1], False))
    when_active(7, 0, BLOCKS, each(gathers[2], False))
    when_active(7, BLOCKS, BLOCKS, each(quarter_copy, False))
    when_active(8, 0, BLOCKS, each(gathers[3], False))
    when_active(9, 0, BLOCKS, each(out_copy, False))

    def elementwise(r, gate, up, dhid):
        rows = pl.ds(r * tb, tb)
        dhid = dhid.astype(BF16).astype(F32)
        s = sigmoid(gate)
        silu = gate * s
        hid_ref[rows, :] = (silu * up).astype(BF16)
        dup_ref[rows, :] = (dhid * silu).astype(BF16)
        dgate_ref[rows, :] = (dhid * up * (s + silu * (1.0 - s))).astype(BF16)

    def weight_terms(r, which):
        rows = pl.ds(r * tb, tb)
        for m, rhs in enumerate((dgate_ref, dup_ref, hid_ref)):
            term = dot(dyt_ref[:, rows] if m == 2 else at_ref[which, :, rows], rhs[rows, :], 1, 0)
            own_term[t % 2, m] = term if r == 0 else own_term[t % 2, m] + term

    @pl.when(t < BLOCKS)
    def _():
        def first(r):
            rows = pl.ds(r * tb, tb)
            gate_buf[r % 2] = dot(a_ref[rows, :], wg_ref[0], 1, 0)
            up_buf[r % 2] = dot(a_ref[rows, :], wu_ref[0], 1, 0)
            dhid_buf[r % 2] = dot(dy_ref[0, rows, :], wd_ref[0], 1, 1)

        def second(r):
            elementwise(r, gate_buf[r % 2], up_buf[r % 2], dhid_buf[r % 2])

        def third(r):
            rows = pl.ds(r * tb, tb)
            by_gate[rows, :] += dot(dgate_ref[rows, :], wg_ref[0], 1, 1)
            by_up[rows, :] += dot(dup_ref[rows, :], wu_ref[0], 1, 1)
            weight_terms(r, 1)

        interleave(tokens // tb, first, second, third)

    @pl.when((t >= BLOCKS) & (t < 2 * BLOCKS))
    def _():
        def first(r):
            dhid_buf[r % 2] = dot(a_ref[pl.ds(r * tb, tb), :], wd_ref[0], 1, 1)

        def second(r):
            rows = pl.ds(r * tb, tb)
            elementwise(r, gate_ref[rows, :], up_ref[rows, :], dhid_buf[r % 2])

        interleave(tokens // tb, first, second, lambda r: weight_terms(r, 0))

    others = range(1, 16)

    def square_copy(k, row):
        return pltpu.make_async_remote_copy(
            all_squares.at[me], all_squares.at[row], sq_send.at[k], sq_recv.at[k],
            device_id={"dp": (me + k) % 16}, device_id_type=pl.DeviceIdType.MESH)

    @pl.when(t == 2 * BLOCKS + 5)
    def _():
        total = squares[0:8, :]
        for r in range(8, squares.shape[0], 8):
            total = total + squares[r : r + 8, :]
        all_squares[me] = total[:, :128] + total[:, 128:]
        for k in others:
            square_copy(k, me).start()

    @pl.when(t == pl.num_programs(0) - 1)
    def _():
        for k in others:
            copy = square_copy(k, (me + 16 - k) % 16)
            copy.wait_send()
            copy.wait_recv()
        total = all_squares[0]
        for k in others:
            total = total + all_squares[k]
        count = 2 * 3 * WHOLE * BLOCK * BLOCKS
        factor = jnp.minimum(1.0, 0.5 * lax.rsqrt(jnp.sum(total, keepdims=True) / count + 1e-30))
        factor_ref[...] = jnp.broadcast_to(factor, factor_ref.shape)


def backward(h, dy, a0t, ws, gate, up, tb=512):
    tokens, d = h.shape
    ff = gate.shape[1]
    assert (d, ff) == (WHOLE, BLOCK * BLOCKS)
    vmem = pl.BlockSpec(memory_space=pltpu.VMEM)
    anywhere = pl.BlockSpec(memory_space=pl.ANY)
    top_block = lambda t: (1, 0, jnp.minimum(t, BLOCKS - 1))
    low_block = lambda t: (0, jnp.minimum(jnp.maximum(t - BLOCKS, 0), BLOCKS - 1))

    def down_block(t):
        t = jnp.minimum(t, 2 * BLOCKS - 1)
        return (1 - t // BLOCKS, t % BLOCKS, 0)

    sizes = [WHOLE >> (i + 1) for i in range(4)]
    return pl.pallas_call(
        functools.partial(backward_kernel, tb),
        grid=(2 * BLOCKS + AT[8],),
        in_specs=[
            vmem, vmem, anywhere,
            pl.BlockSpec((1, d, BLOCK), top_block),
            pl.BlockSpec((1, d, BLOCK), top_block),
            pl.BlockSpec((1, BLOCK, d), down_block),
            pl.BlockSpec((tokens, BLOCK), low_block),
            pl.BlockSpec((tokens, BLOCK), low_block),
        ],
        out_specs=[anywhere] * 6 + [vmem],
        out_shape=[jax.ShapeDtypeStruct((WHOLE, ff), BF16)] * 3 + [jax.ShapeDtypeStruct((BLOCKS, WHOLE // 4, BLOCK), BF16)] * 3 + [jax.ShapeDtypeStruct((8, 128), F32)],
        scratch_shapes=[
            pltpu.VMEM((tokens, d), BF16),
            pltpu.VMEM((2, d, tokens), BF16),
            pltpu.VMEM((d, tokens), BF16),
            pltpu.VMEM((tokens, d), F32),
            pltpu.VMEM((tokens, d), F32),
            pltpu.VMEM((tokens, BLOCK), BF16),
            pltpu.VMEM((tokens, BLOCK), BF16),
            pltpu.VMEM((tokens, BLOCK), BF16),
            *[pltpu.VMEM((2, tb, BLOCK), F32)] * 3,
            pltpu.VMEM((2, 3, WHOLE, BLOCK), F32),
            *[pltpu.VMEM((2, 3, n, BLOCK), F32) for n in sizes[1:]],
            *[pltpu.VMEM((SLOTS, 3, n, BLOCK), BF16) for n in sizes],
            *[pltpu.VMEM((SLOTS, 3, n, BLOCK), BF16) for n in sizes],
            pltpu.VMEM((3, BLOCKS, WHOLE, BLOCK), BF16),
            pltpu.VMEM((sizes[3], BLOCK), F32),
            pltpu.VMEM((16, 8, 128), F32),
            pltpu.SemaphoreType.DMA((4, 3, SLOTS)),
            pltpu.SemaphoreType.DMA((4, 3, SLOTS)),
            pltpu.SemaphoreType.DMA((4, 3, SLOTS)),
            pltpu.SemaphoreType.DMA((4, 3, SLOTS)),
            pltpu.SemaphoreType.DMA((3, 2)),
            pltpu.SemaphoreType.DMA,
            pltpu.SemaphoreType.DMA((16,)),
            pltpu.SemaphoreType.DMA((16,)),
        ],
        compiler_params=pltpu.CompilerParams(vmem_limit_bytes=VMEM_LIMIT, has_side_effects=True),
        cost_estimate=pl.CostEstimate(flops=24 * tokens * d * ff, bytes_accessed=12 * tokens * ff, transcendentals=0),
        name="backward",
    )(h, dy, a0t, *ws, gate, up)


def solution(mesh):
    def step(x, dy, *arrays):
        ws, ms, vs = (arrays[i : i + 3] for i in (0, 3, 6))
        gate, up, h, at = forward(x, *ws)
        *sums, factor = backward(h, dy, at, ws, gate, up)

        def fetch(array, bits):
            return lax.ppermute(array, "dp", [(i, i ^ bits) for i in range(16)])

        pieces = [(q, fetch(q, 1), fetch(q, order[1]), fetch(q, order[1] ^ 1)) for q, order in zip(sums[3:], ORDERS)]
        partly = top_adamw(factor, ws, ms, vs, sums[:3])
        me = lax.axis_index("dp").astype(jnp.int32).reshape(1)
        return tuple(low_adamw(me, factor, ws, ms, vs, pieces, partly))

    return jax.shard_map(
        step,
        mesh=mesh,
        in_specs=(P(("rep", "dp"), None, None),) * 2 + (P(None, None, None),) * 9,
        out_specs=(P("rep", None, None),) * 9,
        check_vma=False,
    )
```

```python
import functools
import jax
import jax.numpy as jnp
from jax import lax
from jax.experimental import pallas as pl
from jax.experimental.pallas import tpu as pltpu
from jax.sharding import PartitionSpec as P

F32, BF16 = jnp.float32, jnp.bfloat16
VMEM_LIMIT = 67_000_000


def dot(a, b, da, db):
    return lax.dot_general(a, b, (((da,), (db,)), ((), ())), preferred_element_type=F32)


def norm_scale(wide):
    return lax.rsqrt(jnp.mean(wide * wide, -1, keepdims=True) + 1e-6)


def sigmoid(g):
    return 1.0 / (1.0 + jnp.exp(-g))


def interleave(n, first, second, third):
    for r in range(n + 2):
        if r < n:
            first(r)
        if 0 <= r - 2:
            third(r - 2)
        if 0 <= r - 1 < n:
            second(r - 1)


def forward_kernel(tb, x_ref, wg_ref, wu_ref, wd_ref, gate_ref, up_ref, h_ref, at_ref, a_ref, acc_ref, hid_ref):
    f, last = pl.program_id(0), pl.num_programs(0) - 1
    tokens = acc_ref.shape[0]

    @pl.when(f == 0)
    def _():
        for t in range(0, tokens, 128):
            rows = pl.ds(t, 128)
            wide = x_ref[0, rows, :].astype(F32)
            a = (wide * norm_scale(wide)).astype(BF16)
            a_ref[rows, :] = a
            at_ref[:, rows] = a.T
            acc_ref[rows, :] = jnp.zeros((128, acc_ref.shape[1]), F32)

    def project(r):
        rows = pl.ds(r * tb, tb)
        gate_ref[rows, :] = dot(a_ref[rows, :], wg_ref[0], 1, 0)
        up_ref[rows, :] = dot(a_ref[rows, :], wu_ref[0], 1, 0)

    def product(r):
        rows = pl.ds(r * tb, tb)
        gate = gate_ref[rows, :]
        hid_ref[rows, :] = (gate * sigmoid(gate) * up_ref[rows, :]).astype(BF16)

    def down(r):
        rows = pl.ds(r * tb, tb)
        acc_ref[rows, :] += dot(hid_ref[rows, :], wd_ref[0], 1, 0)

    interleave(tokens // tb, project, product, down)

    @pl.when(f == last)
    def _():
        for t in range(0, tokens, tb):
            rows = pl.ds(t, tb)
            h_ref[rows, :] = (x_ref[0, rows, :].astype(F32) + acc_ref[rows, :].astype(BF16).astype(F32)).astype(BF16)


def forward(x, wg, wu, wd, fb=512, tb=512):
    _, tokens, d = x.shape
    ff = wg.shape[2]
    whole = lambda *s: pl.BlockSpec(s, lambda f: (0,) * len(s))
    return pl.pallas_call(
        functools.partial(forward_kernel, tb),
        grid=(ff // fb,),
        in_specs=[
            whole(1, tokens, d),
            pl.BlockSpec((1, d, fb), lambda f: (0, 0, f)),
            pl.BlockSpec((1, d, fb), lambda f: (0, 0, f)),
            pl.BlockSpec((1, fb, d), lambda f: (0, f, 0)),
        ],
        out_specs=[
            pl.BlockSpec((tokens, fb), lambda f: (0, f)),
            pl.BlockSpec((tokens, fb), lambda f: (0, f)),
            whole(tokens, d),
            whole(d, tokens),
        ],
        out_shape=[
            jax.ShapeDtypeStruct((tokens, ff), F32),
            jax.ShapeDtypeStruct((tokens, ff), F32),
            jax.ShapeDtypeStruct((tokens, d), BF16),
            jax.ShapeDtypeStruct((d, tokens), BF16),
        ],
        scratch_shapes=[pltpu.VMEM((tokens, d), BF16), pltpu.VMEM((tokens, d), F32), pltpu.VMEM((tokens, fb), BF16)],
        compiler_params=pltpu.CompilerParams(vmem_limit_bytes=VMEM_LIMIT),
        cost_estimate=pl.CostEstimate(flops=6 * tokens * d * ff, bytes_accessed=9 * tokens * ff, transcendentals=0),
        name="forward",
    )(x, wg, wu, wd)


def adamw(w, m, v, g):
    m = 0.9 * m + 0.1 * g
    v = 0.95 * v + 0.05 * g * g
    w = w.astype(F32)
    return (w - 0.02 * (m * lax.rsqrt(v + 1e-8) + 0.1 * w)).astype(BF16), m, v


def top_adamw_kernel(factor_ref, *refs):
    ins, outs = refs[:12], refs[12:]
    for i in range(3):
        w, m, v, g = ins[4 * i : 4 * i + 4]
        g = g[...].astype(F32) * factor_ref[0:1, 0:1]
        for out, new in zip(outs[i::3], adamw(w[0], m[0], v[0], g.T if i == 2 else g)):
            out[0] = new


def low_adamw_kernel(me_ref, factor_ref, *refs):
    ins, outs, scratch = refs[:21], refs[30:39], refs[39:]
    me = me_ref[0]
    for i in range(3):
        w, m, v = ins[7 * i : 7 * i + 3]
        own, across = me % 2, (me // ORDERS[i][1]) % 2
        for k, piece in enumerate(ins[7 * i + 3 : 7 * i + 7]):
            core, chip = (1 - own if k & 1 else own), (1 - across if k & 2 else across)
            rows = pl.ds(pl.multiple_of(core * (WHOLE // 2) + chip * (WHOLE // 4), WHOLE // 4), WHOLE // 4)
            for c in range(piece.shape[0]):
                scratch[i][rows, c * BLOCK : (c + 1) * BLOCK] = piece[c]
        g = scratch[i][...].astype(F32) * factor_ref[0:1, 0:1]
        for out, new in zip(outs[i::3], adamw(w[0], m[0], v[0], g.T if i == 2 else g)):
            out[0] = new


def adamw_parts(layer, steps, ws):
    wide = ws[0].shape[2] // steps
    low = pl.BlockSpec((1, ws[0].shape[1], wide), lambda f: (layer, 0, f))
    down = pl.BlockSpec((1, wide, ws[2].shape[2]), lambda f: (layer, f, 0))
    shapes = [jax.ShapeDtypeStruct(w.shape, t) for t in (BF16, F32, F32) for w in ws]
    return wide, [low, low, down], shapes


def top_adamw(factor, ws, ms, vs, gs, steps=8):
    wide, specs, shapes = adamw_parts(1, steps, ws)
    ins, in_specs = [], []
    for w, m, v, g, spec in zip(ws, ms, vs, gs, specs):
        ins += [w, m, v, g]
        in_specs += [spec] * 3 + [pl.BlockSpec((WHOLE, wide), lambda f: (0, f))]
    return pl.pallas_call(
        top_adamw_kernel,
        grid=(steps,),
        in_specs=[pl.BlockSpec(memory_space=pltpu.VMEM)] + in_specs,
        out_specs=specs * 3,
        out_shape=shapes,
        compiler_params=pltpu.CompilerParams(vmem_limit_bytes=VMEM_LIMIT),
        cost_estimate=pl.CostEstimate(flops=100_000_000_000, bytes_accessed=140_000_000, transcendentals=0),
        name="top_adamw",
    )(factor, *ins)


def low_adamw(me, factor, ws, ms, vs, pieces, partly, steps=8):
    wide, specs, shapes = adamw_parts(0, steps, ws)
    part = pl.BlockSpec((wide // BLOCK, WHOLE // 4, BLOCK), lambda f: (f, 0, 0))
    ins, in_specs = [], []
    for w, m, v, four, spec in zip(ws, ms, vs, pieces, specs):
        ins += [w, m, v, *four]
        in_specs += [spec] * 3 + [part] * 4
    return pl.pallas_call(
        low_adamw_kernel,
        grid=(steps,),
        in_specs=[pl.BlockSpec(memory_space=pltpu.SMEM), pl.BlockSpec(memory_space=pltpu.VMEM)] + in_specs + [pl.BlockSpec(memory_space=pl.ANY)] * 9,
        out_specs=specs * 3,
        out_shape=shapes,
        scratch_shapes=[pltpu.VMEM((WHOLE, wide), BF16)] * 3,
        input_output_aliases={23 + i: i for i in range(9)},
        compiler_params=pltpu.CompilerParams(vmem_limit_bytes=VMEM_LIMIT),
        cost_estimate=pl.CostEstimate(flops=100_000_000_000, bytes_accessed=140_000_000, transcendentals=0),
        name="low_adamw",
    )(me, factor, *ins, *partly)


BLOCK, BLOCKS = 256, 16
WHOLE = 512
SLOTS = 4
TOP_AT = (0, 1, 2, 3, 4, 5, 6, 7, 9, 10, 11)
LOW_AT = (0, 1, 2, 4, 6, 8, 10, 12, 13)
ORDERS = ((1, 8, 4, 2), (1, 4, 2, 8), (1, 2, 8, 4))
MATRICES = range(3)


def backward_kernel(tb, h_ref, dy_ref, a0t_ref, wg_ref, wu_ref, wd_ref, gate_ref, up_ref,
                    g0_ref, g1_ref, g2_ref, q0_ref, q1_ref, q2_ref, factor_ref,
                    a_ref, at_ref, dyt_ref, by_gate, by_up, hid_ref, dgate_ref, dup_ref, gate_buf, up_buf, dhid_buf,
                    own_term, own_half, keep1, keep2, keep3, send1, send2, send3, recv0, recv1, recv2, recv3,
                    gbuf, squares, all_squares, rs_send, rs_recv, ag_send, ag_recv, out_sem, in_sem, sq_send, sq_recv):
    t = pl.program_id(0)
    tokens, d = a_ref.shape
    outs, quarters = (g0_ref, g1_ref, g2_ref), (q0_ref, q1_ref, q2_ref)
    keep, send, recv = (None, keep1, keep2, keep3), (None, send1, send2, send3), (recv0, recv1, recv2, recv3)
    me = lax.axis_index("dp")
    bits = {w: (me // w) % 2 for w in (1, 2, 4, 8)}
    partners = {w: me + w * (1 - 2 * bits[w]) for w in (1, 2, 4, 8)}

    def rs_copy(i, m, slot):
        source = own_half.at[slot, m, half(1 - bits[1], WHOLE // 2), :] if i == 0 else send[i].at[slot, m]
        return pltpu.make_async_remote_copy(
            source, recv[i].at[slot, m], rs_send.at[i, m, slot], rs_recv.at[i, m, slot],
            device_id={"dp": partners[ORDERS[m][i]]}, device_id_type=pl.DeviceIdType.MESH)

    def own_rows(m, phase):
        n = WHOLE >> (phase + 1)
        offset = sum(bits[ORDERS[m][q]] * (WHOLE >> (q + 1)) for q in range(phase + 1))
        return pl.ds(pl.multiple_of(offset, n), n)

    def ag_copy(j, m, b):
        part = gbuf.at[m, b % BLOCKS, own_rows(m, 3 - j), :]
        return pltpu.make_async_remote_copy(
            part, part, ag_send.at[j, m, b % SLOTS], ag_recv.at[j, m, b % SLOTS],
            device_id={"dp": partners[ORDERS[m][3 - j]]}, device_id_type=pl.DeviceIdType.MESH)

    def out_copy(m, b):
        columns = pl.ds(pl.multiple_of((b % BLOCKS) * BLOCK, BLOCK), BLOCK)
        return pltpu.make_async_copy(gbuf.at[m, b % BLOCKS], outs[m].at[:, columns], out_sem.at[m, b % 2])

    def quarter_copy(m, b):
        return pltpu.make_async_copy(gbuf.at[m, b % BLOCKS, own_rows(m, 1), :], quarters[m].at[b % BLOCKS], out_sem.at[m, b % 2])

    def half(bit, n):
        return pl.ds(pl.multiple_of(bit * n, n), n)

    @pl.when(t == 0)
    def _():
        first = pltpu.make_async_copy(a0t_ref, at_ref.at[0], in_sem)
        first.start()
        squares[...] = jnp.zeros_like(squares)
        for r in range(0, tokens, 128):
            rows = pl.ds(r, 128)
            wide = h_ref[rows, :].astype(F32)
            a = (wide * norm_scale(wide)).astype(BF16)
            a_ref[rows, :] = a
            at_ref[1, :, rows] = a.T
            dyt_ref[:, rows] = dy_ref[0, rows, :].T
            by_gate[rows, :] = jnp.zeros((128, d), F32)
            by_up[rows, :] = jnp.zeros((128, d), F32)
        first.wait()

    @pl.when(t == BLOCKS)
    def _():
        for r in range(0, tokens, 128):
            rows = pl.ds(r, 128)
            wide = h_ref[rows, :].astype(F32)
            scale = norm_scale(wide)
            da = (by_gate[rows, :].astype(BF16).astype(F32) + by_up[rows, :].astype(BF16).astype(F32)).astype(BF16).astype(F32)
            dn = scale * da - wide * (scale * scale * scale * jnp.mean(da * wide, -1, keepdims=True))
            dh = (dy_ref[0, rows, :].astype(F32) + dn.astype(BF16).astype(F32)).astype(BF16)
            a_ref[rows, :] = dh
            dyt_ref[:, rows] = dh.T

    def block_at(i):
        if i >= len(LOW_AT):
            return t - TOP_AT[i]
        return jnp.where(t < TOP_AT[i] + BLOCKS, t - TOP_AT[i], jnp.where(t < LOW_AT[i] + BLOCKS, -1, t - LOW_AT[i]))

    def reduce_wait(i):
        for m in MATRICES:
            rs_copy(i - 2, m, block_at(i) % SLOTS).wait()

    def reduce_add(i):
        b = block_at(i)
        slot, pair = b % SLOTS, b % 2
        for m in MATRICES:
            if 2 <= i < 5:
                n, bit = WHOLE >> i, bits[ORDERS[m][i - 1]]
                away, here = half(1 - bit, n), half(bit, n)
                if i == 2:
                    base = bits[ORDERS[m][0]] * 2
                    mine = own_term[pair, m, half(base + 1 - bit, n), :], own_term[pair, m, half(base + bit, n), :]
                else:
                    mine = keep[i - 2][pair, m, away, :], keep[i - 2][pair, m, here, :]
                send[i - 1][slot, m] = (mine[0] + recv[i - 2][slot, m, away, :].astype(F32)).astype(BF16)
                keep[i - 1][pair, m] = mine[1] + recv[i - 2][slot, m, here, :].astype(F32)
            elif i == 5:
                g = (keep[3][pair, m] + recv[3][slot, m].astype(F32)).astype(BF16)
                gbuf[m, b % BLOCKS, own_rows(m, 3), :] = g
                squares[...] += g.astype(F32) * g.astype(F32)

    def reduce_start(i):
        for m in MATRICES:
            rs_copy(i - 1, m, block_at(i) % SLOTS).start()

    def each(copy, wait):
        def act(b):
            for m in MATRICES:
                copy(m, b).wait() if wait else copy(m, b).start()
        return act

    gathers = [functools.partial(ag_copy, j) for j in range(4)]

    def when_active(i, first, count, act):
        b = block_at(i)
        pl.when((b >= first) & (b < first + count))(functools.partial(act, b))

    when_active(10, 0, BLOCKS, each(out_copy, True))
    when_active(9, 0, BLOCKS, each(gathers[3], True))
    when_active(8, 0, BLOCKS, each(gathers[2], True))
    when_active(8, BLOCKS, BLOCKS, each(quarter_copy, True))
    when_active(7, 0, 2 * BLOCKS, each(gathers[1], True))
    when_active(6, 0, 2 * BLOCKS, each(gathers[0], True))
    steady = ((t >= TOP_AT[5]) & (t < BLOCKS + TOP_AT[1])) | ((t >= BLOCKS + LOW_AT[5]) & (t < 2 * BLOCKS + LOW_AT[1]))

    @pl.when(steady)
    def _():
        for i in range(5, 1, -1):
            reduce_wait(i)
        for i in range(5, 1, -1):
            reduce_add(i)
        for i in range(1, 5):
            reduce_start(i)

    @pl.when(jnp.logical_not(steady))
    def _():
        for act, stages in ((reduce_wait, range(5, 1, -1)), (reduce_add, range(5, 1, -1)), (reduce_start, range(1, 5))):
            for i in stages:
                pl.when((block_at(i) >= 0) & (block_at(i) < 2 * BLOCKS))(functools.partial(act, i))

    when_active(5, 0, 2 * BLOCKS, each(gathers[0], False))
    when_active(6, 0, 2 * BLOCKS, each(gathers[1], False))
    when_active(7, 0, BLOCKS, each(gathers[2], False))
    when_active(7, BLOCKS, BLOCKS, each(quarter_copy, False))
    when_active(8, 0, BLOCKS, each(gathers[3], False))
    when_active(9, 0, BLOCKS, each(out_copy, False))

    def elementwise(r, gate, up, dhid):
        rows = pl.ds(r * tb, tb)
        dhid = dhid.astype(BF16).astype(F32)
        s = sigmoid(gate)
        silu = gate * s
        hid_ref[r % 2] = (silu * up).astype(BF16)
        dup_ref[r % 2] = (dhid * silu).astype(BF16)
        dgate_ref[r % 2] = (dhid * up * (s + silu * (1.0 - s))).astype(BF16)

    def weight_terms(r, which):
        rows = pl.ds(r * tb, tb)
        for m, rhs in enumerate((dgate_ref, dup_ref, hid_ref)):
            term = dot(dyt_ref[:, rows] if m == 2 else at_ref[which, :, rows], rhs[r % 2], 1, 0)
            if r > 0:
                term = own_term[t % 2, m] + term
            own_term[t % 2, m] = term
            if r == tokens // tb - 1:
                own_half[t % SLOTS, m] = term.astype(BF16)

    @pl.when(t < BLOCKS)
    def _():
        def first(r):
            rows = pl.ds(r * tb, tb)
            gate_buf[r % 2] = dot(a_ref[rows, :], wg_ref[0], 1, 0)
            up_buf[r % 2] = dot(a_ref[rows, :], wu_ref[0], 1, 0)
            dhid_buf[r % 2] = dot(dy_ref[0, rows, :], wd_ref[0], 1, 1)

        def second(r):
            elementwise(r, gate_buf[r % 2], up_buf[r % 2], dhid_buf[r % 2])

        def third(r):
            rows = pl.ds(r * tb, tb)
            by_gate[rows, :] += dot(dgate_ref[r % 2], wg_ref[0], 1, 1)
            by_up[rows, :] += dot(dup_ref[r % 2], wu_ref[0], 1, 1)
            weight_terms(r, 1)

        interleave(tokens // tb, first, second, third)

    @pl.when((t >= BLOCKS) & (t < 2 * BLOCKS))
    def _():
        def first(r):
            dhid_buf[r % 2] = dot(a_ref[pl.ds(r * tb, tb), :], wd_ref[0], 1, 1)

        def second(r):
            rows = pl.ds(r * tb, tb)
            elementwise(r, gate_ref[rows, :], up_ref[rows, :], dhid_buf[r % 2])

        interleave(tokens // tb, first, second, lambda r: weight_terms(r, 0))

    others = range(1, 16)

    def square_copy(k, row):
        return pltpu.make_async_remote_copy(
            all_squares.at[me], all_squares.at[row], sq_send.at[k], sq_recv.at[k],
            device_id={"dp": (me + k) % 16}, device_id_type=pl.DeviceIdType.MESH)

    @pl.when(t == 2 * BLOCKS + LOW_AT[5])
    def _():
        total = squares[0:8, :]
        for r in range(8, squares.shape[0], 8):
            total = total + squares[r : r + 8, :]
        all_squares[me] = total[:, :128] + total[:, 128:]
        for k in others:
            square_copy(k, me).start()

    @pl.when(t == pl.num_programs(0) - 1)
    def _():
        for k in others:
            copy = square_copy(k, (me + 16 - k) % 16)
            copy.wait_send()
            copy.wait_recv()
        total = all_squares[0]
        for k in others:
            total = total + all_squares[k]
        count = 2 * 3 * WHOLE * BLOCK * BLOCKS
        factor = jnp.minimum(1.0, 0.5 * lax.rsqrt(jnp.sum(total, keepdims=True) / count + 1e-30))
        factor_ref[...] = jnp.broadcast_to(factor, factor_ref.shape)


def backward(h, dy, a0t, ws, gate, up, tb=512):
    tokens, d = h.shape
    ff = gate.shape[1]
    assert (d, ff) == (WHOLE, BLOCK * BLOCKS)
    vmem = pl.BlockSpec(memory_space=pltpu.VMEM)
    anywhere = pl.BlockSpec(memory_space=pl.ANY)
    top_block = lambda t: (1, 0, jnp.minimum(t, BLOCKS - 1))
    low_block = lambda t: (0, jnp.minimum(jnp.maximum(t - BLOCKS, 0), BLOCKS - 1))

    def down_block(t):
        t = jnp.minimum(t, 2 * BLOCKS - 1)
        return (1 - t // BLOCKS, t % BLOCKS, 0)

    sizes = [WHOLE >> (i + 1) for i in range(4)]
    return pl.pallas_call(
        functools.partial(backward_kernel, tb),
        grid=(2 * BLOCKS + LOW_AT[8],),
        in_specs=[
            vmem, vmem, anywhere,
            pl.BlockSpec((1, d, BLOCK), top_block),
            pl.BlockSpec((1, d, BLOCK), top_block),
            pl.BlockSpec((1, BLOCK, d), down_block),
            pl.BlockSpec((tokens, BLOCK), low_block),
            pl.BlockSpec((tokens, BLOCK), low_block),
        ],
        out_specs=[anywhere] * 6 + [vmem],
        out_shape=[jax.ShapeDtypeStruct((WHOLE, ff), BF16)] * 3 + [jax.ShapeDtypeStruct((BLOCKS, WHOLE // 4, BLOCK), BF16)] * 3 + [jax.ShapeDtypeStruct((8, 128), F32)],
        scratch_shapes=[
            pltpu.VMEM((tokens, d), BF16),
            pltpu.VMEM((2, d, tokens), BF16),
            pltpu.VMEM((d, tokens), BF16),
            pltpu.VMEM((tokens, d), F32),
            pltpu.VMEM((tokens, d), F32),
            pltpu.VMEM((2, tb, BLOCK), BF16),
            pltpu.VMEM((2, tb, BLOCK), BF16),
            pltpu.VMEM((2, tb, BLOCK), BF16),
            *[pltpu.VMEM((2, tb, BLOCK), F32)] * 3,
            pltpu.VMEM((2, 3, WHOLE, BLOCK), F32),
            pltpu.VMEM((SLOTS, 3, WHOLE, BLOCK), BF16),
            *[pltpu.VMEM((2, 3, n, BLOCK), F32) for n in sizes[1:]],
            *[pltpu.VMEM((SLOTS, 3, n, BLOCK), BF16) for n in sizes[1:]],
            *[pltpu.VMEM((SLOTS, 3, n, BLOCK), BF16) for n in sizes],
            pltpu.VMEM((3, BLOCKS, WHOLE, BLOCK), BF16),
            pltpu.VMEM((sizes[3], BLOCK), F32),
            pltpu.VMEM((16, 8, 128), F32),
            pltpu.SemaphoreType.DMA((4, 3, SLOTS)),
            pltpu.SemaphoreType.DMA((4, 3, SLOTS)),
            pltpu.SemaphoreType.DMA((4, 3, SLOTS)),
            pltpu.SemaphoreType.DMA((4, 3, SLOTS)),
            pltpu.SemaphoreType.DMA((3, 2)),
            pltpu.SemaphoreType.DMA,
            pltpu.SemaphoreType.DMA((16,)),
            pltpu.SemaphoreType.DMA((16,)),
        ],
        compiler_params=pltpu.CompilerParams(vmem_limit_bytes=VMEM_LIMIT, has_side_effects=True),
        cost_estimate=pl.CostEstimate(flops=24 * tokens * d * ff, bytes_accessed=12 * tokens * ff, transcendentals=0),
        name="backward",
    )(h, dy, a0t, *ws, gate, up)


def solution(mesh):
    def step(x, dy, *arrays):
        ws, ms, vs = (arrays[i : i + 3] for i in (0, 3, 6))
        gate, up, h, at = forward(x, *ws)
        *sums, factor = backward(h, dy, at, ws, gate, up)

        def fetch(array, bits):
            return lax.ppermute(array, "dp", [(i, i ^ bits) for i in range(16)])

        pieces = [(q, fetch(q, 1), fetch(q, order[1]), fetch(q, order[1] ^ 1)) for q, order in zip(sums[3:], ORDERS)]
        partly = top_adamw(factor, ws, ms, vs, sums[:3])
        me = lax.axis_index("dp").astype(jnp.int32).reshape(1)
        return tuple(low_adamw(me, factor, ws, ms, vs, pieces, partly))

    return jax.shard_map(
        step,
        mesh=mesh,
        in_specs=(P(("rep", "dp"), None, None),) * 2 + (P(None, None, None),) * 9,
        out_specs=(P("rep", None, None),) * 9,
        check_vma=False,
    )
```
